32 devices in a mesh: tm: 8 (over z, x), space: 4 (over y, core).
Axes of the slice: x: 2, y: 2, z: 4, core: 2. Of those that a mesh axis runs over, the one named last changes fastest.
Arguments:
- u_old: float32 [8, 5, 256, 16, 128], P('tm', None, 'space'), may hold values from -2.5 to 2.5
- u_init: float32 [256, 16, 128], P('space'), may hold values from -2.5 to 2.5
Outputs:
- u_new: float32 [8, 5, 256, 16, 128], P('tm', None, 'space')
The draws below stay inside these ranges and needn't reach their ends.
All inputs are finite; a program needn't handle non-finite values.
Results may differ from the reference program's by a relative error of at most 0.0003.
Values sent between devices are 32-bit elements; how exact they have to be, the bound alone decides.
A program may use at most 128 MiB of HBM per device.

```python
import math
import jax
import jax.numpy as jnp
from jax import lax

NZ = 256
NX = 16
NY = 128
FINE_NODES = 5
SLICES = 8
N_TM = 8


def steps_of(key, extent, pieces, smallest, high):
    factor_of, own = 1.0, jax.random.fold_in(key, 6)
    for dim, shards_of in pieces:
        draws = jnp.exp(jax.random.uniform(jax.random.fold_in(own, dim), (shards_of,), jnp.float32, smallest / len(pieces), high / len(pieces)))
        factor_of = factor_of * jnp.repeat(draws, extent[dim] // shards_of).reshape([-1 if axis == dim else 1 for axis in range(len(extent))])
    return factor_of


def bell_draw(own_key, extent, spread, most, split=(), held_as=jnp.bfloat16):
    drawn = jax.random.normal(own_key, extent, jnp.float32) * spread
    if len(split) > 0:
        drawn = steps_of(own_key, extent, split, -0.22, 0.18) * drawn
    return jnp.clip(drawn, min=-most, max=most).astype(held_as)


def setup_inputs(seed: int = 0) -> dict:
    key_of = jax.random.split(jax.random.key(seed), 3)
    return {
        "u_old": bell_draw(key_of[0], (SLICES, FINE_NODES, NZ, NX, NY), 0.6, 2.5, ((0, 8), (2, 4)), jnp.float32),
        "u_init": bell_draw(key_of[1], (NZ, NX, NY), 0.6, 2.5, ((0, 4),), jnp.float32),
    }


step_length = 0.4
diffusion = 1.0
reaction = 1.0

def basis_coefficients(nodes, chosen):
    polynomial = [1.0]
    for other, point in enumerate(nodes):
        if other == chosen:
            continue
        divisor = nodes[chosen] - point
        widened = [0.0] * (len(polynomial) + 1)
        for power, value in enumerate(polynomial):
            widened[power + 1] += value / divisor
            widened[power] -= value * point / divisor
        polynomial = widened
    return polynomial

def basis_value(nodes, chosen, where):
    result = 1.0
    for other, point in enumerate(nodes):
        if other != chosen:
            result *= (where - point) / (nodes[chosen] - point)
    return result

def node_tables():
    root = math.sqrt(3.0 / 7.0)
    fine_tau = [0.0, (1.0 - root) / 2.0, 0.5, (1.0 + root) / 2.0, 1.0]
    coarse_tau = [0.0, 0.5, 1.0]
    integ = []
    for j in range(4):
        row_values = []
        for k in range(5):
            polynomial = basis_coefficients(fine_tau, k)
            total = 0.0
            for power, value in enumerate(polynomial):
                total += value * (fine_tau[j + 1] ** (power + 1) - fine_tau[j] ** (power + 1)) / (power + 1)
            row_values.append(total)
        integ.append(row_values)
    interp = [[basis_value(coarse_tau, c, fine_tau[m]) for c in range(3)] for m in range(5)]
    spacing = [float(fine_tau[j + 1] - fine_tau[j]) for j in range(4)]
    return (jnp.asarray(integ, jnp.float32), spacing, jnp.asarray(interp, jnp.float32))

def fine_force(field):
    near = jnp.roll(field, 1, 0) + jnp.roll(field, -1, 0) + jnp.roll(field, 1, 1) + jnp.roll(field, -1, 1)
    near = near + jnp.roll(field, 1, 2) + jnp.roll(field, -1, 2)
    return diffusion * (near - 6.0 * field) + reaction * (field - field * field * field)

def coarse_lap(field):
    near = jnp.roll(field, 1, 0) + jnp.roll(field, -1, 0) + jnp.roll(field, 1, 1) + jnp.roll(field, -1, 1)
    near = near + jnp.roll(field, 1, 2) + jnp.roll(field, -1, 2)
    return 0.25 * (near - 6.0 * field)

def restrict(field):
    depth, rows, cols = field.shape
    return field.reshape(depth // 2, 2, rows // 2, 2, cols // 2, 2).mean(axis=(1, 3, 5))

def reference(u_old, u_init):
    integ, spacing, interp = node_tables()
    depth_c, rows_c, cols_c = (NZ // 2, NX // 2, NY // 2)
    angle_z = 2.0 * jnp.cos(2.0 * jnp.pi * jnp.arange(depth_c, dtype=jnp.float32) / depth_c)
    angle_x = 2.0 * jnp.cos(2.0 * jnp.pi * jnp.arange(rows_c, dtype=jnp.float32) / rows_c)
    angle_y = 2.0 * jnp.cos(2.0 * jnp.pi * jnp.arange(cols_c, dtype=jnp.float32) / cols_c)
    eigen = 0.25 * (angle_z[:, None, None] + angle_x[None, :, None] + angle_y[None, None, :] - 6.0)
    denom = 1.0 - 0.5 * step_length * diffusion * eigen

    def solve(right):
        return jnp.real(jnp.fft.ifftn(jnp.fft.fftn(right) / denom)).astype(jnp.float32)
    carry = restrict(u_init)
    results = []
    for slice_index in range(N_TM):
        fine_old = u_old[slice_index]
        start = u_init if slice_index == 0 else u_old[slice_index - 1, 4]
        fold = jnp.stack([fine_force(fine_old[k]) for k in range(5)])
        iold = step_length * jnp.einsum('jk,kzxy->jzxy', integ, fold, precision=lax.Precision.HIGHEST)
        states = [start]
        forces = []
        for section in range(4):
            force_now = fine_force(states[section])
            forces.append(force_now)
            states.append(states[section] + step_length * spacing[section] * (force_now - fold[section]) + iold[section])
        forces.append(fine_force(states[4]))
        inew = step_length * jnp.einsum('jk,kzxy->jzxy', integ, jnp.stack(forces), precision=lax.Precision.HIGHEST)
        coarse = [restrict(states[0]), restrict(states[2]), restrict(states[4])]
        lifted0 = restrict(inew[0] + inew[1]) - 0.5 * step_length * diffusion * coarse_lap(coarse[1])
        lifted1 = restrict(inew[2] + inew[3]) - 0.5 * step_length * diffusion * coarse_lap(coarse[2])
        begin = carry
        middle = solve(begin + lifted0)
        finish = solve(middle + lifted1)
        carry = finish
        delta = jnp.stack([begin - coarse[0], middle - coarse[1], finish - coarse[2]])
        timed = jnp.einsum('mc,czxy->mzxy', interp, delta, precision=lax.Precision.HIGHEST)
        upper = jnp.repeat(jnp.repeat(jnp.repeat(timed, 2, 1), 2, 2), 2, 3)
        results.append(jnp.stack(states) + upper)
    return jnp.stack(results)
```

```python
import functools
import math

import jax
import jax.numpy as jnp
import numpy as np
from jax import lax
from jax.experimental import pallas as pl
from jax.experimental.pallas import tpu as pltpu
from jax.sharding import PartitionSpec as P

step_length = 0.4
diffusion = 1.0
reaction = 1.0
HALO = 5
BLOCK = 4
PARTS = 4
MESH = pl.DeviceIdType.MESH


def basis_coefficients(nodes, chosen):
    polynomial = [1.0]
    for other, point in enumerate(nodes):
        if other == chosen:
            continue
        divisor = nodes[chosen] - point
        widened = [0.0] * (len(polynomial) + 1)
        for power, value in enumerate(polynomial):
            widened[power + 1] += value / divisor
            widened[power] -= value * point / divisor
        polynomial = widened
    return polynomial


def basis_value(nodes, chosen, where):
    result = 1.0
    for other, point in enumerate(nodes):
        if other != chosen:
            result *= (where - point) / (nodes[chosen] - point)
    return result


def node_tables():
    root = math.sqrt(3.0 / 7.0)
    fine_tau = [0.0, (1.0 - root) / 2.0, 0.5, (1.0 + root) / 2.0, 1.0]
    coarse_tau = [0.0, 0.5, 1.0]
    integ = []
    for j in range(4):
        row_values = []
        for k in range(5):
            polynomial = basis_coefficients(fine_tau, k)
            total = 0.0
            for power, value in enumerate(polynomial):
                total += (
                    value
                    * (fine_tau[j + 1] ** (power + 1) - fine_tau[j] ** (power + 1))
                    / (power + 1)
                )
            row_values.append(total)
        integ.append(row_values)
    interp = [[basis_value(coarse_tau, c, fine_tau[m]) for c in range(3)] for m in range(5)]
    spacing = [float(fine_tau[j + 1] - fine_tau[j]) for j in range(4)]
    return integ, spacing, interp


def hartley(length):
    counter = np.arange(length)
    phase = 2.0 * np.pi * (counter[:, None] * counter[None, :] % length) / length
    return (np.cos(phase) + np.sin(phase)) / math.sqrt(length)


def two_parts(table):
    upper = table.astype(jnp.bfloat16)
    lower = (table - upper.astype(np.float64)).astype(jnp.bfloat16)
    return np.stack([upper, lower])


def halves(value):
    upper = value.astype(jnp.bfloat16)
    return upper, (value - upper.astype(jnp.float32)).astype(jnp.bfloat16)


def product(a, b, dims):
    def one(x, y):
        return lax.dot_general(x, y, (dims, ((), ())), preferred_element_type=jnp.float32)

    return one(a[0], b[0]) + (one(a[0], b[1]) + one(a[1], b[0]))


def force(padded):
    field = padded[1:-1]
    rows, cols = field.shape[1:]
    near = padded[2:] + padded[:-2]
    near = near + (pltpu.roll(field, 1, 1) + pltpu.roll(field, rows - 1, 1))
    near = near + (pltpu.roll(field, 1, 2) + pltpu.roll(field, cols - 1, 2))
    linear = reaction - 6.0 * diffusion
    return diffusion * near + field * (linear - reaction * (field * field))


def kernel(
    nt, ns, solvers,
    u_hbm, init_hbm, tab_hbm, ztab_hbm, inv_hbm,
    w, up,
    u, corr, acc, restricted, tab, ztab, inv,
    send_1, recv_1, send_2, recv_2,
    load_sem, table_sem, start_sem, halo_send, halo_recv, start_send, start_recv,
    sems, known_sem,
):
    integ, spacing, interp = node_tables()
    h = step_length
    devices = nt * ns
    depth, rows, cols = init_hbm.shape
    depth_c, rows_c = depth // 2, rows // 2
    length = send_1.shape[2]
    modes = send_1.shape[1]
    own = pl.ds(HALO, depth)
    t, s = lax.axis_index("tm"), lax.axis_index("space")
    me = t * ns + s
    above, below = lax.rem(s + 1, ns), lax.rem(s + ns - 1, ns)

    barrier = pltpu.get_barrier_semaphore()

    def signal_along(sem, step):
        @pl.when(t + step < nt)
        def _():
            pl.semaphore_signal(sem, inc=1, device_id=(t + step, s), device_id_type=MESH)

        @pl.when(t >= step)
        def _():
            pl.semaphore_signal(sem, inc=1, device_id=(t - step, s), device_id_type=MESH)

    def sides(step):
        return jnp.where(t + step < nt, 1, 0) + jnp.where(t >= step, 1, 0)

    signal_along(barrier, 1)
    for i in range(1, ns):
        pl.semaphore_signal(
            barrier, inc=1, device_id=(t, lax.rem(s + i, ns)), device_id_type=MESH
        )
    load = pltpu.make_async_copy(u_hbm.at[0], u.at[:, own], load_sem)
    load.start()
    tables = [
        pltpu.make_async_copy(source, target, table_sem.at[i])
        for i, (source, target) in enumerate(((tab_hbm, tab), (ztab_hbm, ztab), (inv_hbm, inv)))
    ]
    for copy in tables:
        copy.start()
    local_start = pltpu.make_async_copy(init_hbm, w.at[0, own], start_sem)

    @pl.when(t == 0)
    def _():
        local_start.start()

    pl.semaphore_wait(barrier, ns - 1 + sides(1))

    lows, highs = pl.ds(0, HALO), pl.ds(HALO + depth, HALO)
    first, last = pl.ds(0, HALO), pl.ds(depth - HALO, HALO)

    def remote(source, target, send, recv, place):
        return pltpu.make_async_remote_copy(
            src_ref=source, dst_ref=target, send_sem=send, recv_sem=recv,
            device_id=place, device_id_type=MESH,
        )

    after = jnp.minimum(t + 1, nt - 1)
    node = u_hbm.at[0, 4]
    cuts = [(0, HALO), (depth - HALO, HALO), (HALO, depth - 2 * HALO)]
    starts = [
        remote(
            node.at[pl.ds(begin, size)], w.at[0, pl.ds(HALO + begin, size)],
            start_send.at[i], start_recv.at[i], (after, s),
        )
        for i, (begin, size) in enumerate(cuts)
    ]

    def edges(source, shift):
        return [
            remote(
                source.at[pl.ds(shift + depth - HALO, HALO)], w.at[0, lows],
                start_send.at[3], start_recv.at[3], (t, above),
            ),
            remote(
                source.at[pl.ds(shift, HALO)], w.at[0, highs],
                start_send.at[4], start_recv.at[4], (t, below),
            ),
        ]

    inits, passed = edges(init_hbm, 0), edges(w.at[0], HALO)
    halos = [
        remote(u_hbm.at[0, :, last], u.at[:, lows], halo_send.at[0], halo_recv.at[0], (t, above)),
        remote(u_hbm.at[0, :, first], u.at[:, highs], halo_send.at[1], halo_recv.at[1], (t, below)),
    ]
    @pl.when(t < nt - 1)
    def _():
        for copy in starts:
            copy.start()

    for copy in halos:
        copy.start()

    @pl.when(t == 0)
    def _():
        for copy in inits:
            copy.start()

    signal_along(known_sem.at[0], 1)
    load.wait()
    for copy in halos:
        copy.wait_recv()

    blocks = (depth + 2 * HALO - 2) // BLOCK

    def fold_block(i, carry):
        z = 1 + i * BLOCK
        forces = [force(u[k, pl.ds(z - 1, BLOCK + 2)]) for k in range(5)]
        for j in range(4):
            total = None
            for k in range(5):
                weight = h * integ[j][k] - (h * spacing[j] if j == k else 0.0)
                term = weight * forces[k]
                total = term if total is None else total + term
            corr[j, pl.ds(z, BLOCK)] = total
        return carry

    lax.fori_loop(0, blocks, fold_block, 0)

    @pl.when(t == 0)
    def _():
        local_start.wait()

    @pl.when(t > 0)
    def _():
        starts[1].wait_recv()
        passed[0].start()
        starts[0].wait_recv()
        passed[1].start()

    for i in range(known_sem.shape[0]):
        if i > 0:
            signal_along(known_sem.at[i], 2 ** i)
        pl.semaphore_wait(known_sem.at[i], sides(2 ** i))

    @pl.when(t > 0)
    def _():
        starts[2].wait_recv()

    for copy in inits:
        copy.wait_recv()

    for m in range(4):
        def sweep_block(i, carry, m=m):
            z = 1 + i * BLOCK
            here = pl.ds(z, BLOCK)
            padded = w[m, pl.ds(z - 1, BLOCK + 2)]
            now = force(padded)
            w[m + 1, here] = padded[1:-1] + (h * spacing[m]) * now + corr[m, here]
            for a in range(2):
                term = (h * (integ[2 * a][m] + integ[2 * a + 1][m])) * now
                acc[a, here] = term if m == 0 else acc[a, here] + term
            return carry

        lax.fori_loop(0, blocks, sweep_block, 0)

    plane = rows * depth_c

    def last_block(i, carry):
        z = HALO + i * BLOCK
        here = pl.ds(z, BLOCK)
        padded = w[4, pl.ds(z - 1, BLOCK + 2)]
        now, end = force(padded), padded[1:-1]
        middle = w[2, here]
        outs = []
        for a in range(2):
            term = acc[a, here] + (h * (integ[2 * a][4] + integ[2 * a + 1][4])) * now
            outs.append(term + ((w[0, here] - middle) if a == 0 else (middle - end)))
        outs.append(end - u[4, here])
        for f in range(3):
            pair = outs[f].reshape(BLOCK // 2, 2, rows, cols)
            pair = pair[:, 0] + pair[:, 1]
            place = pl.multiple_of(f * plane + i * (BLOCK // 2) * rows, 8)
            restricted[pl.ds(place, BLOCK // 2 * rows), :] = pair.reshape(BLOCK // 2 * rows, cols)
        return carry

    lax.fori_loop(0, depth // BLOCK, last_block, 0)

    filled = 3 * depth_c
    pieces = []
    for x in range(rows_c):
        even = restricted[pl.ds(2 * x, filled, stride=rows), :]
        odd = restricted[pl.ds(2 * x + 1, filled, stride=rows), :]
        pieces.append((even + odd) * 0.125)
    flat = jnp.concatenate(pieces, axis=1)
    if length > filled:
        flat = jnp.concatenate([flat, jnp.zeros((length - filled, rows_c * cols), jnp.float32)], axis=0)
    for copy in tables:
        copy.wait()
    spectral = product((tab[0], tab[1]), halves(flat), ((1,), (1,)))
    send_1[...] = spectral.reshape(solvers, modes, length)

    slot = s * nt + t

    def spread(i, carry):
        other = lax.rem(me + i, solvers)

        @pl.when(other != me)
        def _():
            remote(
                send_1.at[other], recv_1.at[slot], sems.at[0], sems.at[1],
                (other // ns, lax.rem(other, ns)),
            ).start()

        return carry

    lax.fori_loop(0, solvers, spread, 0)

    def when_all(condition, body):
        if solvers == devices:
            body()
        else:
            pl.when(condition)(body)

    def bytes_wait(ref, count, sem):
        part = ref.at[pl.ds(0, count)]
        pltpu.make_async_copy(part, part, sem).wait()

    def solve():
        recv_1[slot] = send_1[me]
        bytes_wait(recv_1, devices - 1, sems.at[1])
        joined = jnp.concatenate(
            [recv_1[pl.ds(q * nt, nt)].reshape(nt * modes, length) for q in range(ns)], axis=1
        )
        spectra = product(halves(joined), (ztab[0], ztab[1]), ((1,), (0,)))
        width = inv.shape[1]
        factor = inv[pl.ds(pl.multiple_of(me * modes, 8), modes), :]
        begin = jnp.zeros((modes, width), jnp.float32)
        rows_of = []
        for n in range(nt):
            part = spectra[n * modes:(n + 1) * modes]
            middle = (begin + part[:, :width]) * factor
            finish = (middle + part[:, width:2 * width]) * factor
            rows_of.append(jnp.concatenate([begin, middle, finish], axis=1))
            begin = finish + part[:, 2 * width:]
        solved = jnp.concatenate(rows_of, axis=0)
        back = product(halves(solved), (ztab[0], ztab[1]), ((1,), (1,)))
        for q in range(ns):
            send_2[pl.ds(q * nt, nt)] = back[:, q * length:(q + 1) * length].reshape(nt, modes, length)

        def give(i, carry):
            other = lax.rem(me + i, devices)
            to_t, to_s = other // ns, lax.rem(other, ns)
            remote(
                send_2.at[to_s * nt + to_t], recv_2.at[me], sems.at[2], sems.at[3], (to_t, to_s)
            ).start()
            return carry

        lax.fori_loop(1, devices, give, 0)
        recv_2[me] = send_2[slot]
        bytes_wait(recv_2, solvers - 1, sems.at[3])

    when_all(me < solvers, solve)
    if solvers != devices:
        @pl.when(me >= solvers)
        def _():
            bytes_wait(recv_2, solvers, sems.at[3])

    delta = jnp.transpose(recv_2[...].reshape(solvers * modes, length))[:filled]
    coarse = product(halves(delta), (tab[0], tab[1]), ((1,), (0,)))
    for x in range(rows_c):
        part = coarse[:, x * cols:(x + 1) * cols]
        for side in range(2):
            up[pl.ds(2 * x + side, filled, stride=rows), :] = part

    for copy in halos:
        copy.wait_send()

    @pl.when(t < nt - 1)
    def _():
        for copy in starts:
            copy.wait_send()

    for copy in inits:
        copy.wait_send()

    def sent():
        bytes_wait(send_1, solvers - 1, sems.at[0])
        bytes_wait(send_2, devices - 1, sems.at[2])

    when_all(me < solvers, sent)
    if solvers != devices:
        @pl.when(me >= solvers)
        def _():
            bytes_wait(send_1, solvers, sems.at[0])


def finish(w, up, out, staged, sems):
    _, _, interp = node_tables()
    depth, rows, cols = out.shape[2:]
    plane = rows * (depth // 2)
    part = depth // PARTS

    def give(p):
        return pltpu.make_async_copy(staged.at[p], out.at[0, :, pl.ds(p * part, part)], sems.at[p])

    for p in range(PARTS):
        def add_block(i, carry, p=p):
            begin = p * part + i * BLOCK
            count = BLOCK // 2 * rows
            fields = [
                up[pl.ds(pl.multiple_of(c * plane + begin // 2 * rows, 8), count), :] for c in range(3)
            ]
            for m in range(5):
                total = None
                for c in range(3):
                    if abs(interp[m][c]) < 1e-14:
                        continue
                    term = fields[c]
                    if abs(interp[m][c] - 1.0) > 1e-14:
                        term = interp[m][c] * term
                    total = term if total is None else total + term
                total = total.reshape(BLOCK // 2, 1, rows, cols)
                total = jnp.broadcast_to(total, (BLOCK // 2, 2, rows, cols)).reshape(BLOCK, rows, cols)
                staged[p, m, pl.ds(i * BLOCK, BLOCK)] = w[m, pl.ds(HALO + begin, BLOCK)] + total
            return carry

        lax.fori_loop(0, part // BLOCK, add_block, 0)
        give(p).start()
    for p in range(PARTS):
        give(p).wait()


def shards(nt, ns, u_old, u_init):
    depth, rows, cols = u_init.shape
    depth_c, rows_c, cols_c = depth // 2, rows // 2, cols // 2
    whole_c = depth_c * ns
    count = rows_c * cols_c
    devices = nt * ns
    solvers = min(devices, count // 8)
    modes = count // solvers
    length = -(-3 * depth_c // 128) * 128
    extended = depth + 2 * HALO
    rounds = max(1, (nt - 1).bit_length())

    wide = np.repeat(hartley(cols_c), 2, axis=1)
    tab = two_parts(np.kron(hartley(rows_c), wide))
    wave = hartley(whole_c)
    ztab = np.zeros((ns, length, 3 * whole_c))
    for f in range(3):
        ztab[:, f * depth_c:(f + 1) * depth_c, f * whole_c:(f + 1) * whole_c] = wave.reshape(ns, depth_c, whole_c)
    ztab = two_parts(ztab.reshape(ns * length, 3 * whole_c))
    angle_z = 2.0 * np.cos(2.0 * np.pi * np.arange(whole_c) / whole_c)
    angle_x = 2.0 * np.cos(2.0 * np.pi * np.arange(rows_c) / rows_c)
    angle_y = 2.0 * np.cos(2.0 * np.pi * np.arange(cols_c) / cols_c)
    planar = (angle_x[:, None] + angle_y[None, :]).reshape(count)
    eigen = 0.25 * (planar[:, None] + angle_z[None, :] - 6.0)
    inv = (1.0 / (1.0 - 0.5 * step_length * diffusion * eigen)).astype(np.float32)

    f32 = jnp.float32
    states, corrections = pl.pallas_call(
        functools.partial(kernel, nt, ns, solvers),
        out_shape=(
            jax.ShapeDtypeStruct((5, extended, rows, cols), f32),
            jax.ShapeDtypeStruct((3 * depth_c * rows, cols), f32),
        ),
        in_specs=[pl.BlockSpec(memory_space=pltpu.HBM)] * 5,
        out_specs=(pl.BlockSpec(memory_space=pltpu.VMEM),) * 2,
        scratch_shapes=[
            pltpu.VMEM((5, extended, rows, cols), f32),
            pltpu.VMEM((4, extended, rows, cols), f32),
            pltpu.VMEM((2, extended, rows, cols), f32),
            pltpu.VMEM((3 * depth_c * rows, cols), f32),
            pltpu.VMEM(tab.shape, jnp.bfloat16),
            pltpu.VMEM(ztab.shape, jnp.bfloat16),
            pltpu.VMEM(inv.shape, f32),
            pltpu.VMEM((solvers, modes, length), f32),
            pltpu.VMEM((devices, modes, length), f32),
            pltpu.VMEM((devices, modes, length), f32),
            pltpu.VMEM((solvers, modes, length), f32),
            pltpu.SemaphoreType.DMA,
            pltpu.SemaphoreType.DMA((3,)),
            pltpu.SemaphoreType.DMA,
            pltpu.SemaphoreType.DMA((2,)),
            pltpu.SemaphoreType.DMA((2,)),
            pltpu.SemaphoreType.DMA((5,)),
            pltpu.SemaphoreType.DMA((5,)),
            pltpu.SemaphoreType.DMA((4,)),
            pltpu.SemaphoreType.REGULAR((rounds,)),
        ],
        compiler_params=pltpu.CompilerParams(
            collective_id=0, has_side_effects=True, vmem_limit_bytes=30000000
        ),
    )(*(pltpu.with_memory_space_constraint(a, pltpu.HBM) for a in (u_old, u_init, tab, ztab, inv)))
    return pl.pallas_call(
        finish,
        out_shape=jax.ShapeDtypeStruct((1, 5, depth, rows, cols), f32),
        in_specs=[pl.BlockSpec(memory_space=pltpu.VMEM)] * 2,
        out_specs=pl.BlockSpec(memory_space=pltpu.HBM),
        scratch_shapes=[
            pltpu.VMEM((PARTS, 5, depth // PARTS, rows, cols), f32),
            pltpu.SemaphoreType.DMA((PARTS,)),
        ],
        compiler_params=pltpu.CompilerParams(vmem_limit_bytes=16000000),
    )(states, corrections)


def solution(mesh):
    return jax.shard_map(
        functools.partial(shards, mesh.shape["tm"], mesh.shape["space"]),
        mesh=mesh,
        in_specs=(P("tm", None, "space", None, None), P("space", None, None)),
        out_specs=P("tm", None, "space", None, None),
        check_vma=False,
    )
```

```python
import functools
import math

import jax
import jax.numpy as jnp
import numpy as np
from jax import lax
from jax.experimental import pallas as pl
from jax.experimental.pallas import tpu as pltpu
from jax.sharding import PartitionSpec as P

step_length = 0.4
diffusion = 1.0
reaction = 1.0
HALO = 5
BLOCK = 8
PIECE = 4
PARTS = 4
GROUPS = 2
MESH = pl.DeviceIdType.MESH


def basis_coefficients(nodes, chosen):
    polynomial = [1.0]
    for other, point in enumerate(nodes):
        if other == chosen:
            continue
        divisor = nodes[chosen] - point
        widened = [0.0] * (len(polynomial) + 1)
        for power, value in enumerate(polynomial):
            widened[power + 1] += value / divisor
            widened[power] -= value * point / divisor
        polynomial = widened
    return polynomial


def basis_value(nodes, chosen, where):
    result = 1.0
    for other, point in enumerate(nodes):
        if other != chosen:
            result *= (where - point) / (nodes[chosen] - point)
    return result


def node_tables():
    root = math.sqrt(3.0 / 7.0)
    fine_tau = [0.0, (1.0 - root) / 2.0, 0.5, (1.0 + root) / 2.0, 1.0]
    coarse_tau = [0.0, 0.5, 1.0]
    integ = []
    for j in range(4):
        row_values = []
        for k in range(5):
            polynomial = basis_coefficients(fine_tau, k)
            total = 0.0
            for power, value in enumerate(polynomial):
                total += (
                    value
                    * (fine_tau[j + 1] ** (power + 1) - fine_tau[j] ** (power + 1))
                    / (power + 1)
                )
            row_values.append(total)
        integ.append(row_values)
    interp = [[basis_value(coarse_tau, c, fine_tau[m]) for c in range(3)] for m in range(5)]
    spacing = [float(fine_tau[j + 1] - fine_tau[j]) for j in range(4)]
    return integ, spacing, interp


def hartley(length):
    counter = np.arange(length)
    phase = 2.0 * np.pi * (counter[:, None] * counter[None, :] % length) / length
    return (np.cos(phase) + np.sin(phase)) / math.sqrt(length)


def two_parts(table):
    upper = table.astype(jnp.bfloat16)
    lower = (table - upper.astype(np.float64)).astype(jnp.bfloat16)
    return np.stack([upper, lower])


def halves(value):
    upper = value.astype(jnp.bfloat16)
    return upper, (value - upper.astype(jnp.float32)).astype(jnp.bfloat16)


def product(a, b, dims):
    def one(x, y):
        return lax.dot_general(x, y, (dims, ((), ())), preferred_element_type=jnp.float32)

    return one(a[0], b[0]) + (one(a[0], b[1]) + one(a[1], b[0]))


def force(padded):
    field = padded[1:-1]
    rows, cols = field.shape[1:]
    near = padded[2:] + padded[:-2]
    near = near + (pltpu.roll(field, 1, 1) + pltpu.roll(field, rows - 1, 1))
    near = near + (pltpu.roll(field, 1, 2) + pltpu.roll(field, cols - 1, 2))
    linear = reaction - 6.0 * diffusion
    return diffusion * near + field * (linear - reaction * (field * field))


def kernel(
    nt, ns, groups,
    u_hbm, init_hbm, ytab_hbm, xtab_hbm, ztab_hbm, inv_hbm,
    w, up,
    u, corr, forces, restricted, ytab, ytab_back, xtab, ztab, inv,
    send_1, recv_1, send_2, recv_2, carry_out, carry_in,
    load_sem, table_sem, start_sem, halo_send, halo_recv, start_send, start_recv,
    sems, known_sem,
):
    integ, spacing, _ = node_tables()
    h = step_length
    depth, rows, cols = init_hbm.shape
    depth_c, rows_c = depth // 2, rows // 2
    half = rows_c // 2
    width = send_1.shape[1]
    length = send_1.shape[2]
    solvers = width // 8
    span = nt // groups
    own = pl.ds(HALO, depth)
    t, s = lax.axis_index("tm"), lax.axis_index("space")
    group = t // span
    base = group * span
    above, below = lax.rem(s + 1, ns), lax.rem(s + ns - 1, ns)
    per = max(1, solvers // ns)
    lead = base + (span - per) // 2
    mine = (t - lead) * ns + s
    is_solver = (t >= lead) & (mine < solvers)
    all_solve = solvers == span * ns

    def place_of(a):
        return lead + a // ns, lax.rem(a, ns)

    barrier = pltpu.get_barrier_semaphore()

    def signal_along(sem, step):
        @pl.when(t + step < nt)
        def _():
            pl.semaphore_signal(sem, inc=1, device_id=(t + step, s), device_id_type=MESH)

        @pl.when(t >= step)
        def _():
            pl.semaphore_signal(sem, inc=1, device_id=(t - step, s), device_id_type=MESH)

    def sides(step):
        return jnp.where(t + step < nt, 1, 0) + jnp.where(t >= step, 1, 0)

    signal_along(barrier, 1)
    for i in range(1, ns):
        pl.semaphore_signal(
            barrier, inc=1, device_id=(t, lax.rem(s + i, ns)), device_id_type=MESH
        )
    load = pltpu.make_async_copy(u_hbm.at[0], u.at[:, own], load_sem)
    load.start()
    tables = [
        pltpu.make_async_copy(source, target, table_sem.at[i])
        for i, (source, target) in enumerate(
            ((ytab_hbm.at[0], ytab), (ytab_hbm.at[1], ytab_back), (xtab_hbm, xtab), (ztab_hbm, ztab), (inv_hbm, inv))
        )
    ]
    for copy in tables:
        copy.start()
    local_start = pltpu.make_async_copy(init_hbm, w.at[0, own], start_sem)

    @pl.when(t == 0)
    def _():
        local_start.start()

    with jax.named_scope("barrier"):
        pl.semaphore_wait(barrier, ns - 1 + sides(1))

    lows, highs = pl.ds(0, HALO), pl.ds(HALO + depth, HALO)
    first, last = pl.ds(0, HALO), pl.ds(depth - HALO, HALO)

    def remote(source, target, send, recv, place):
        return pltpu.make_async_remote_copy(
            src_ref=source, dst_ref=target, send_sem=send, recv_sem=recv,
            device_id=place, device_id_type=MESH,
        )

    after = jnp.minimum(t + 1, nt - 1)
    node = u_hbm.at[0, 4]
    steps = depth // BLOCK - 2

    def start_piece(i, begin, size):
        return remote(
            node.at[pl.ds(begin, size)], w.at[0, pl.ds(HALO + begin, size)],
            start_send.at[i], start_recv.at[i], (after, s),
        )

    def inner(i):
        return start_piece(4 + i, HALO + i * BLOCK, BLOCK)

    start_edges = [start_piece(0, 0, HALO), start_piece(1, depth - HALO, HALO)]
    final = start_piece(4 + steps, HALO + steps * BLOCK, depth - 2 * HALO - steps * BLOCK)
    starts = start_edges + [inner(i) for i in range(steps)] + [final]

    def edges(source, shift):
        return [
            remote(
                source.at[pl.ds(shift + depth - HALO, HALO)], w.at[0, lows],
                start_send.at[2], start_recv.at[2], (t, above),
            ),
            remote(
                source.at[pl.ds(shift, HALO)], w.at[0, highs],
                start_send.at[3], start_recv.at[3], (t, below),
            ),
        ]

    inits, passed = edges(init_hbm, 0), edges(w.at[0], HALO)
    halos = [
        remote(u_hbm.at[0, :, last], u.at[:, lows], halo_send.at[0], halo_recv.at[0], (t, above)),
        remote(u_hbm.at[0, :, first], u.at[:, highs], halo_send.at[1], halo_recv.at[1], (t, below)),
    ]

    @pl.when(t < nt - 1)
    def _():
        for copy in starts:
            copy.start()

    for copy in halos:
        copy.start()

    @pl.when(t == 0)
    def _():
        for copy in inits:
            copy.start()

    signal_along(known_sem.at[0], 1)
    rounds = known_sem.shape[0]

    def hear(i):
        pl.semaphore_wait(known_sem.at[i], sides(2 ** i))
        if i + 1 < rounds:
            signal_along(known_sem.at[i + 1], 2 ** (i + 1))

    with jax.named_scope("w_edges"):
        @pl.when(t > 0)
        def _():
            start_edges[1].wait_recv()
            passed[0].start()
            start_edges[0].wait_recv()
            passed[1].start()

    if rounds > 1:
        hear(0)

    with jax.named_scope("w_halo"):
        load.wait()
        for copy in halos:
            copy.wait_recv()

    if rounds > 2:
        hear(1)

    def fold_block(i, carry):
        z = 1 + i * BLOCK
        parts = [force(u[k, pl.ds(z - 1, BLOCK + 2)]) for k in range(5)]
        for j in range(4):
            total = None
            for k in range(5):
                weight = h * integ[j][k] - (h * spacing[j] if j == k else 0.0)
                term = weight * parts[k]
                total = term if total is None else total + term
            corr[j, pl.ds(z, BLOCK)] = total
        return carry

    with jax.named_scope("fold"):
        lax.fori_loop(0, (depth + 2 * HALO - 2) // BLOCK, fold_block, 0)

    for i in range(2, rounds - 1):
        hear(i)

    @pl.when(t == 0)
    def _():
        local_start.wait()

    for copy in inits:
        copy.wait_recv()

    def advance(m, padded, here):
        now = force(padded)
        forces[m, here] = now
        result = padded[1:-1] + (h * spacing[m]) * now + corr[m, here]
        w[m + 1, here] = result
        return result

    plane = rows * depth_c

    def step(begin, count):
        reached = None
        for m in range(5):
            at = begin - m
            if m == 0:
                padded = w[0, pl.ds(at - 1, count + 2)]
            else:
                padded = jnp.concatenate([w[m, pl.ds(at - 1, 2)], reached], axis=0)
            if m < 4:
                reached = advance(m, padded, pl.ds(at, count))
        here = pl.ds(at, count)
        now, end = force(padded), padded[1:-1]
        middle = w[2, here]
        olds = [forces[m, here] for m in range(4)] + [now]
        outs = []
        for a in range(2):
            total = (w[0, here] - middle) if a == 0 else (middle - end)
            for m in range(5):
                total = total + (h * (integ[2 * a][m] + integ[2 * a + 1][m])) * olds[m]
            outs.append(total)
        outs.append(end - u[4, here])
        for f in range(3):
            pair = outs[f].reshape(count // 2, 2, rows, cols)
            pair = pair[:, 0] + pair[:, 1]
            to = f * plane + (at - HALO) // 2 * rows
            if not isinstance(to, int):
                to = pl.multiple_of(to, 8)
            restricted[pl.ds(to, count // 2 * rows), :] = pair.reshape(count // 2 * rows, cols)

    with jax.named_scope("prologue"):
        for m in range(4):
            count = BLOCK - 2 * m
            advance(m, w[m, pl.ds(m, count + 2)], pl.ds(1 + m, count))

    def main_step(i, carry):
        @pl.when(t > 0)
        def _():
            inner(i).wait_recv()

        step(HALO + 4 + i * BLOCK, BLOCK)
        return carry

    with jax.named_scope("steps"):
        lax.fori_loop(0, steps, main_step, 0)

    with jax.named_scope("w_final"):
        @pl.when(t > 0)
        def _():
            final.wait_recv()

    with jax.named_scope("tail"):
        step(HALO + 4 + steps * BLOCK, 2 * BLOCK)

    with jax.named_scope("fwd"):
        filled = 3 * depth_c
        for copy in tables:
            copy.wait()
        slabs = []
        for x in range(rows_c):
            even = restricted[pl.ds(2 * x, filled, stride=rows), :]
            odd = restricted[pl.ds(2 * x + 1, filled, stride=rows), :]
            slabs.append(even + odd)
        pairs = [
            jnp.concatenate([slabs[x] + slabs[x + half], slabs[x] - slabs[x + half]], axis=1)
            for x in range(half)
        ]
        turned = product(halves(jnp.concatenate(pairs, axis=0)), (ytab[0], ytab[1]), ((1,), (0,)))
        parts = [turned[x * filled:(x + 1) * filled] for x in range(half)]
        mixed = []
        for j in range(half):
            total = None
            for x in range(half):
                term = xtab[pl.ds(j * half + x, 1), :] * parts[x]
                total = term if total is None else total + term
            mixed.append(total)
        for f in range(3):
            field = jnp.concatenate([mixed[j][f * depth_c:(f + 1) * depth_c] for j in range(half)], axis=0)
            if length > half * depth_c:
                field = jnp.concatenate([field, jnp.zeros((length - half * depth_c, width), jnp.float32)], axis=0)
            send_1[f] = jnp.transpose(field)

    slot = s * span + (t - base)
    hear(rounds - 1)

    def spread(i, carry):
        a = lax.rem(s * per + i, solvers)
        to_t, to_s = place_of(a)

        @pl.when((to_t != t) | (to_s != s))
        def _():
            remote(
                send_1.at[:, pl.ds(pl.multiple_of(a * 8, 8), 8)], recv_1.at[slot],
                sems.at[0], sems.at[1], (to_t, to_s),
            ).start()

        return carry

    with jax.named_scope("issue1"):
        lax.fori_loop(0, solvers, spread, 0)

    def when_solver(body):
        if all_solve:
            body()
        else:
            pl.when(is_solver)(body)

    def bytes_wait(ref, count, sem):
        if count > 0:
            part = ref.at[pl.ds(0, count)]
            pltpu.make_async_copy(part, part, sem).wait()

    def carry_copy(to_t):
        return remote(carry_out, carry_in, sems.at[4], sems.at[5], (to_t, s))

    def solve():
        at = pl.multiple_of(mine * 8, 8)
        recv_1[slot] = send_1[:, pl.ds(at, 8)]
        factor = inv[pl.ds(at, 8), :]
        with jax.named_scope("w_recv1"):
            bytes_wait(recv_1, span * ns - 1, sems.at[1])
        with jax.named_scope("solve"):
            joined = jnp.concatenate(
                [
                    jnp.concatenate(
                        [recv_1[pl.ds(q * span, span), f].reshape(span * 8, length) for q in range(ns)], axis=1
                    )
                    for f in range(3)
                ],
                axis=0,
            )
            spectra = product(halves(joined), (ztab[0], ztab[1]), ((1,), (0,)))
            height = span * 8

            if groups > 1:
                carry_in_zero = group == 0

                @pl.when(carry_in_zero)
                def _():
                    carry_in[...] = jnp.zeros(carry_in.shape, jnp.float32)

                @pl.when(group > 0)
                def _():
                    carry_copy(t).wait_recv()

                begin = carry_in[...]
            else:
                begin = jnp.zeros(factor.shape, jnp.float32)
            fields = [[], [], []]
            for n in range(span):
                part = [spectra[f * height + n * 8:f * height + n * 8 + 8] for f in range(3)]
                middle = (begin + part[0]) * factor
                finish = (middle + part[1]) * factor
                for f, value in enumerate((begin, middle, finish)):
                    fields[f].append(value)
                begin = finish + part[2]
            if groups > 1:
                carry_out[...] = begin

                @pl.when(group < groups - 1)
                def _():
                    carry_copy(t + span).start()

            solved = jnp.concatenate([value for field in fields for value in field], axis=0)
            back = product(halves(solved), (ztab[0], ztab[1]), ((1,), (1,)))
            for f in range(3):
                for q in range(ns):
                    send_2[pl.ds(q * span, span), f] = back[
                        f * height:(f + 1) * height, q * length:(q + 1) * length
                    ].reshape(span, 8, length)

        def give(i, carry):
            other = lax.rem(slot + i, span * ns)
            remote(
                send_2.at[other], recv_2.at[mine], sems.at[2], sems.at[3],
                (base + lax.rem(other, span), other // span),
            ).start()
            return carry

        with jax.named_scope("issue2"):
            lax.fori_loop(1, span * ns, give, 0)
        recv_2[mine] = send_2[slot]
        with jax.named_scope("w_recv2"):
            bytes_wait(recv_2, solvers - 1, sems.at[3])

    when_solver(solve)
    if not all_solve:
        @pl.when(jnp.logical_not(is_solver))
        def _():
            with jax.named_scope("w_recv2"):
                bytes_wait(recv_2, solvers, sems.at[3])

    with jax.named_scope("inv"):
        returned = [jnp.transpose(recv_2[:, f].reshape(width, length)) for f in range(3)]
        mixed = [
            jnp.concatenate([returned[f][j * depth_c:(j + 1) * depth_c] for f in range(3)], axis=0)
            for j in range(half)
        ]
        parts = []
        for x in range(half):
            total = None
            for j in range(half):
                term = xtab[pl.ds(j * half + x, 1), :] * mixed[j]
                total = term if total is None else total + term
            parts.append(total)
        coarse = product(halves(jnp.concatenate(parts, axis=0)), (ytab_back[0], ytab_back[1]), ((1,), (1,)))
        for x in range(rows_c):
            part = coarse[(x % half) * filled:(x % half + 1) * filled, (x // half) * cols:(x // half + 1) * cols]
            for side in range(2):
                up[pl.ds(2 * x + side, filled, stride=rows), :] = part

    for copy in halos:
        copy.wait_send()

    @pl.when(t < nt - 1)
    def _():
        for copy in starts:
            copy.wait_send()

    for copy in inits:
        copy.wait_send()

    def sent():
        bytes_wait(recv_1, solvers - 1, sems.at[0])
        bytes_wait(send_2, span * ns - 1, sems.at[2])
        if groups > 1:
            @pl.when(group < groups - 1)
            def _():
                carry_copy(t).wait_send()

    when_solver(sent)
    if not all_solve:
        @pl.when(jnp.logical_not(is_solver))
        def _():
            bytes_wait(recv_2, solvers, sems.at[0])


def finish(w, up, out, staged, sems):
    _, _, interp = node_tables()
    depth, rows, cols = out.shape[2:]
    plane = rows * (depth // 2)
    part = depth // PARTS

    def give(p):
        return pltpu.make_async_copy(staged.at[p], out.at[0, :, pl.ds(p * part, part)], sems.at[p])

    for p in range(PARTS):
        def add_block(i, carry, p=p):
            begin = p * part + i * PIECE
            count = PIECE // 2 * rows
            fields = [
                up[pl.ds(pl.multiple_of(c * plane + begin // 2 * rows, 8), count), :] for c in range(3)
            ]
            for m in range(5):
                total = None
                for c in range(3):
                    if abs(interp[m][c]) < 1e-14:
                        continue
                    term = fields[c]
                    if abs(interp[m][c] - 1.0) > 1e-14:
                        term = interp[m][c] * term
                    total = term if total is None else total + term
                total = total.reshape(PIECE // 2, 1, rows, cols)
                total = jnp.broadcast_to(total, (PIECE // 2, 2, rows, cols)).reshape(PIECE, rows, cols)
                staged[p, m, pl.ds(i * PIECE, PIECE)] = w[m, pl.ds(HALO + begin, PIECE)] + total
            return carry

        lax.fori_loop(0, part // PIECE, add_block, 0)
        give(p).start()
    for p in range(PARTS):
        give(p).wait()


def shards(nt, ns, u_old, u_init):
    depth, rows, cols = u_init.shape
    depth_c, rows_c, cols_c = depth // 2, rows // 2, cols // 2
    half = rows_c // 2
    whole_c = depth_c * ns
    width = 2 * cols_c
    solvers = width // 8
    groups = GROUPS
    span = nt // groups
    length = -(-half * depth_c // 128) * 128
    extended = depth + 2 * HALO
    rounds = max(1, (nt - 1).bit_length())
    steps = depth // BLOCK - 2

    wide = np.repeat(hartley(cols_c), 2, axis=0)
    zero = np.zeros_like(wide)
    forth = 0.125 * np.block([[wide, zero], [zero, wide]])
    back = np.block([[wide, wide], [wide, -wide]])
    ytab = np.stack([two_parts(forth), two_parts(back)])
    wave_x = hartley(rows_c)
    xtab = np.zeros((half * half, width), np.float32)
    for j in range(half):
        for x in range(half):
            xtab[j * half + x, :cols_c] = wave_x[2 * j, x]
            xtab[j * half + x, cols_c:] = wave_x[2 * j + 1, x]
    wave_z = hartley(whole_c).reshape(ns, depth_c, whole_c)
    ztab = np.zeros((ns, length, half, whole_c))
    for j in range(half):
        ztab[:, j * depth_c:(j + 1) * depth_c, j] = wave_z
    ztab = two_parts(ztab.reshape(ns * length, half * whole_c))
    angle_z = 2.0 * np.cos(2.0 * np.pi * np.arange(whole_c) / whole_c)
    angle_x = 2.0 * np.cos(2.0 * np.pi * np.arange(rows_c) / rows_c)
    angle_y = 2.0 * np.cos(2.0 * np.pi * np.arange(cols_c) / cols_c)
    eigen = 0.25 * (
        angle_x.reshape(half, 2).T[:, None, :, None] + angle_y[None, :, None, None] + angle_z - 6.0
    )
    inv = (1.0 / (1.0 - 0.5 * step_length * diffusion * eigen)).astype(np.float32)
    inv = inv.reshape(width, half * whole_c)

    f32 = jnp.float32
    arrays = (u_old, u_init, ytab, xtab, ztab, inv)
    states, corrections = pl.pallas_call(
        functools.partial(kernel, nt, ns, groups),
        out_shape=(
            jax.ShapeDtypeStruct((5, extended, rows, cols), f32),
            jax.ShapeDtypeStruct((3 * depth_c * rows, cols), f32),
        ),
        in_specs=[pl.BlockSpec(memory_space=pltpu.HBM)] * 6,
        out_specs=(pl.BlockSpec(memory_space=pltpu.VMEM),) * 2,
        scratch_shapes=[
            pltpu.VMEM((5, extended, rows, cols), f32),
            pltpu.VMEM((4, extended, rows, cols), f32),
            pltpu.VMEM((4, extended, rows, cols), f32),
            pltpu.VMEM((3 * depth_c * rows, cols), f32),
            pltpu.VMEM(ytab.shape[1:], jnp.bfloat16),
            pltpu.VMEM(ytab.shape[1:], jnp.bfloat16),
            pltpu.VMEM(xtab.shape, f32),
            pltpu.VMEM(ztab.shape, jnp.bfloat16),
            pltpu.VMEM(inv.shape, f32),
            pltpu.VMEM((3, width, length), f32),
            pltpu.VMEM((span * ns, 3, 8, length), f32),
            pltpu.VMEM((span * ns, 3, 8, length), f32),
            pltpu.VMEM((solvers, 3, 8, length), f32),
            pltpu.VMEM((8, half * whole_c), f32),
            pltpu.VMEM((8, half * whole_c), f32),
            pltpu.SemaphoreType.DMA,
            pltpu.SemaphoreType.DMA((5,)),
            pltpu.SemaphoreType.DMA,
            pltpu.SemaphoreType.DMA((2,)),
            pltpu.SemaphoreType.DMA((2,)),
            pltpu.SemaphoreType.DMA((5 + steps,)),
            pltpu.SemaphoreType.DMA((5 + steps,)),
            pltpu.SemaphoreType.DMA((6,)),
            pltpu.SemaphoreType.REGULAR((rounds,)),
        ],
        compiler_params=pltpu.CompilerParams(
            collective_id=0, has_side_effects=True, vmem_limit_bytes=36000000
        ),
    )(*(pltpu.with_memory_space_constraint(a, pltpu.HBM) for a in arrays))
    return pl.pallas_call(
        finish,
        out_shape=jax.ShapeDtypeStruct((1, 5, depth, rows, cols), f32),
        in_specs=[pl.BlockSpec(memory_space=pltpu.VMEM)] * 2,
        out_specs=pl.BlockSpec(memory_space=pltpu.HBM),
        scratch_shapes=[
            pltpu.VMEM((PARTS, 5, depth // PARTS, rows, cols), f32),
            pltpu.SemaphoreType.DMA((PARTS,)),
        ],
        compiler_params=pltpu.CompilerParams(vmem_limit_bytes=16000000),
    )(states, corrections)


def solution(mesh):
    return jax.shard_map(
        functools.partial(shards, mesh.shape["tm"], mesh.shape["space"]),
        mesh=mesh,
        in_specs=(P("tm", None, "space", None, None), P("space", None, None)),
        out_specs=P("tm", None, "space", None, None),
        check_vma=False,
    )
```

```python
import functools
import math

import jax
import jax.numpy as jnp
import numpy as np
from jax import lax
from jax.experimental import pallas as pl
from jax.experimental.pallas import tpu as pltpu
from jax.sharding import PartitionSpec as P

step_length = 0.4
diffusion = 1.0
reaction = 1.0
HALO = 5
BLOCK = 8
GROUPS = 2
MESH = pl.DeviceIdType.MESH


def basis_coefficients(nodes, chosen):
    polynomial = [1.0]
    for other, point in enumerate(nodes):
        if other == chosen:
            continue
        divisor = nodes[chosen] - point
        widened = [0.0] * (len(polynomial) + 1)
        for power, value in enumerate(polynomial):
            widened[power + 1] += value / divisor
            widened[power] -= value * point / divisor
        polynomial = widened
    return polynomial


def basis_value(nodes, chosen, where):
    result = 1.0
    for other, point in enumerate(nodes):
        if other != chosen:
            result *= (where - point) / (nodes[chosen] - point)
    return result


def node_tables():
    root = math.sqrt(3.0 / 7.0)
    fine_tau = [0.0, (1.0 - root) / 2.0, 0.5, (1.0 + root) / 2.0, 1.0]
    coarse_tau = [0.0, 0.5, 1.0]
    integ = []
    for j in range(4):
        row_values = []
        for k in range(5):
            polynomial = basis_coefficients(fine_tau, k)
            total = 0.0
            for power, value in enumerate(polynomial):
                total += (
                    value
                    * (fine_tau[j + 1] ** (power + 1) - fine_tau[j] ** (power + 1))
                    / (power + 1)
                )
            row_values.append(total)
        integ.append(row_values)
    interp = [[basis_value(coarse_tau, c, fine_tau[m]) for c in range(3)] for m in range(5)]
    spacing = [float(fine_tau[j + 1] - fine_tau[j]) for j in range(4)]
    return integ, spacing, interp


def hartley(length):
    counter = np.arange(length)
    phase = 2.0 * np.pi * (counter[:, None] * counter[None, :] % length) / length
    return (np.cos(phase) + np.sin(phase)) / math.sqrt(length)


def two_parts(table):
    upper = table.astype(jnp.bfloat16)
    lower = (table - upper.astype(np.float64)).astype(jnp.bfloat16)
    return np.stack([upper, lower])


def halves(value):
    upper = value.astype(jnp.bfloat16)
    return upper, (value - upper.astype(jnp.float32)).astype(jnp.bfloat16)


def product(a, b, dims):
    def one(x, y):
        return lax.dot_general(x, y, (dims, ((), ())), preferred_element_type=jnp.float32)

    return one(a[0], b[0]) + (one(a[0], b[1]) + one(a[1], b[0]))


def far_first(flip):
    hops = bin(flip[0]).count("1") + bin(flip[1] // 2).count("1")
    return -(flip[1] // 2), -hops, -flip[0]


def force(padded):
    field = padded[1:-1]
    rows, cols = field.shape[1:]
    near = padded[2:] + padded[:-2]
    near = near + (pltpu.roll(field, 1, 1) + pltpu.roll(field, rows - 1, 1))
    near = near + (pltpu.roll(field, 1, 2) + pltpu.roll(field, cols - 1, 2))
    linear = reaction - 6.0 * diffusion
    return diffusion * near + field * (linear - reaction * (field * field))


def kernel(
    nt, ns, groups,
    u_hbm, init_hbm, ytab_hbm, xtab_hbm, zback_hbm, zearly_hbm, zlate_hbm, inv_hbm,
    w, recv_2, ytab_back, xtab,
    u, corr, forces, restricted, ytab, zback, zearly, zlate, inv,
    send_a, recv_a, staged, send_l, recv_l, send_2, carry_out, carry_in,
    load_sem, table_sem, start_sem, halo_send, halo_recv, start_send, start_recv,
    sems, known_sem,
):
    integ, spacing, _ = node_tables()
    h = step_length
    depth, rows, cols = init_hbm.shape
    depth_c, rows_c = depth // 2, rows // 2
    half = rows_c // 2
    width = staged.shape[1]
    length = send_2.shape[3]
    late_c = BLOCK
    blocks = length // (half * late_c)
    middles = 1 if depth_c > 2 * late_c else 0
    early_c = depth_c - (1 + middles) * late_c
    tiles = send_a.shape[0]
    solvers = width // 8
    span = nt // groups
    own = pl.ds(HALO, depth)
    t, s = lax.axis_index("tm"), lax.axis_index("space")
    group = t // span
    base = group * span
    above, below = lax.rem(s + 1, ns), lax.rem(s + ns - 1, ns)
    per = max(1, solvers // ns)
    lead = base + (span - per) // 2
    mine = (t - lead) * ns + s
    is_solver = (t >= lead) & (mine < solvers)
    all_solve = solvers == span * ns

    def place_of(a):
        return lead + a // ns, lax.rem(a, ns)

    barrier = pltpu.get_barrier_semaphore()

    def signal_along(sem, step):
        @pl.when(t + step < nt)
        def _():
            pl.semaphore_signal(sem, inc=1, device_id=(t + step, s), device_id_type=MESH)

        @pl.when(t >= step)
        def _():
            pl.semaphore_signal(sem, inc=1, device_id=(t - step, s), device_id_type=MESH)

    def sides(step):
        return jnp.where(t + step < nt, 1, 0) + jnp.where(t >= step, 1, 0)

    signal_along(barrier, 1)
    for i in range(1, ns):
        pl.semaphore_signal(
            barrier, inc=1, device_id=(t, lax.rem(s + i, ns)), device_id_type=MESH
        )
    load = pltpu.make_async_copy(u_hbm.at[0], u.at[:, own], load_sem)
    load.start()
    tables = [
        pltpu.make_async_copy(source, target, table_sem.at[i])
        for i, (source, target) in enumerate(
            (
                (ytab_hbm.at[0], ytab), (ytab_hbm.at[1], ytab_back), (xtab_hbm, xtab), (zback_hbm, zback),
                (zearly_hbm, zearly), (zlate_hbm, zlate), (inv_hbm, inv),
            )
        )
    ]
    for copy in tables:
        copy.start()
    local_start = pltpu.make_async_copy(init_hbm, w.at[0, own], start_sem)

    @pl.when(t == 0)
    def _():
        local_start.start()

    with jax.named_scope("barrier"):
        pl.semaphore_wait(barrier, ns - 1 + sides(1))

    lows, highs = pl.ds(0, HALO), pl.ds(HALO + depth, HALO)
    first, last = pl.ds(0, HALO), pl.ds(depth - HALO, HALO)

    def remote(source, target, send, recv, place):
        return pltpu.make_async_remote_copy(
            src_ref=source, dst_ref=target, send_sem=send, recv_sem=recv,
            device_id=place, device_id_type=MESH,
        )

    after = jnp.minimum(t + 1, nt - 1)
    node = u_hbm.at[0, 4]
    steps = depth // BLOCK - 2

    def start_piece(i, begin, size):
        return remote(
            node.at[pl.ds(begin, size)], w.at[0, pl.ds(HALO + begin, size)],
            start_send.at[i], start_recv.at[i], (after, s),
        )

    def inner(i):
        return start_piece(4 + i, HALO + i * BLOCK, BLOCK)

    start_edges = [start_piece(0, 0, HALO), start_piece(1, depth - HALO, HALO)]
    final = start_piece(4 + steps, HALO + steps * BLOCK, depth - 2 * HALO - steps * BLOCK)
    starts = start_edges + [inner(i) for i in range(steps)] + [final]

    def edges(source, shift):
        return [
            remote(
                source.at[pl.ds(shift + depth - HALO, HALO)], w.at[0, lows],
                start_send.at[2], start_recv.at[2], (t, above),
            ),
            remote(
                source.at[pl.ds(shift, HALO)], w.at[0, highs],
                start_send.at[3], start_recv.at[3], (t, below),
            ),
        ]

    inits, passed = edges(init_hbm, 0), edges(w.at[0], HALO)
    halos = [
        remote(u_hbm.at[0, :, last], u.at[:, lows], halo_send.at[0], halo_recv.at[0], (t, above)),
        remote(u_hbm.at[0, :, first], u.at[:, highs], halo_send.at[1], halo_recv.at[1], (t, below)),
    ]

    @pl.when(t < nt - 1)
    def _():
        for copy in starts:
            copy.start()

    for copy in halos:
        copy.start()

    @pl.when(t == 0)
    def _():
        for copy in inits:
            copy.start()

    signal_along(known_sem.at[0], 1)
    rounds = known_sem.shape[0]

    def hear(i):
        pl.semaphore_wait(known_sem.at[i], sides(2 ** i))
        if i + 1 < rounds:
            signal_along(known_sem.at[i + 1], 2 ** (i + 1))

    with jax.named_scope("w_edges"):
        @pl.when(t > 0)
        def _():
            start_edges[1].wait_recv()
            passed[0].start()
            start_edges[0].wait_recv()
            passed[1].start()

    if rounds > 1:
        hear(0)

    with jax.named_scope("w_halo"):
        load.wait()
        for copy in halos:
            copy.wait_recv()

    if rounds > 2:
        hear(1)

    def fold_block(i, carry):
        z = 1 + i * BLOCK
        parts = [force(u[k, pl.ds(z - 1, BLOCK + 2)]) for k in range(5)]
        for j in range(4):
            total = None
            for k in range(5):
                weight = h * integ[j][k] - (h * spacing[j] if j == k else 0.0)
                term = weight * parts[k]
                total = term if total is None else total + term
            corr[j, pl.ds(z, BLOCK)] = total
        return carry

    with jax.named_scope("fold"):
        lax.fori_loop(0, (depth + 2 * HALO - 2) // BLOCK, fold_block, 0)

    for i in range(2, rounds - 1):
        hear(i)

    @pl.when(t == 0)
    def _():
        local_start.wait()

    for copy in inits:
        copy.wait_recv()

    def advance(m, padded, here):
        now = force(padded)
        forces[m, here] = now
        result = padded[1:-1] + (h * spacing[m]) * now + corr[m, here]
        w[m + 1, here] = result
        return result

    plane = rows * depth_c

    def step(begin, count):
        reached = None
        for m in range(5):
            at = begin - m
            if m == 0:
                padded = w[0, pl.ds(at - 1, count + 2)]
            else:
                padded = jnp.concatenate([w[m, pl.ds(at - 1, 2)], reached], axis=0)
            if m < 4:
                reached = advance(m, padded, pl.ds(at, count))
        here = pl.ds(at, count)
        now, end = force(padded), padded[1:-1]
        middle = w[2, here]
        olds = [forces[m, here] for m in range(4)] + [now]
        outs = []
        for a in range(2):
            total = (w[0, here] - middle) if a == 0 else (middle - end)
            for m in range(5):
                total = total + (h * (integ[2 * a][m] + integ[2 * a + 1][m])) * olds[m]
            outs.append(total)
        outs.append(end - u[4, here])
        for f in range(3):
            pair = outs[f].reshape(count // 2, 2, rows, cols)
            pair = pair[:, 0] + pair[:, 1]
            to = f * plane + (at - HALO) // 2 * rows
            if not isinstance(to, int):
                to = pl.multiple_of(to, 8)
            restricted[pl.ds(to, count // 2 * rows), :] = pair.reshape(count // 2 * rows, cols)

    with jax.named_scope("prologue"):
        for m in range(4):
            count = BLOCK - 2 * m
            advance(m, w[m, pl.ds(m, count + 2)], pl.ds(1 + m, count))

    def main_step(i, carry):
        @pl.when(t > 0)
        def _():
            inner(i).wait_recv()

        step(HALO + 4 + i * BLOCK, BLOCK)
        return carry

    def transformed(begin, count):
        slabs = []
        for x in range(rows_c):
            fields = []
            for f in range(3):
                at = f * plane + begin * rows + 2 * x
                even = restricted[pl.ds(at, count, stride=rows), :]
                odd = restricted[pl.ds(at + 1, count, stride=rows), :]
                fields.append(even + odd)
            slabs.append(jnp.concatenate(fields, axis=0))
        pairs = [
            jnp.concatenate([slabs[x] + slabs[x + half], slabs[x] - slabs[x + half]], axis=1)
            for x in range(half)
        ]
        turned = product(halves(jnp.concatenate(pairs, axis=0)), (ytab[0], ytab[1]), ((1,), (0,)))
        parts = [turned[x * 3 * count:(x + 1) * 3 * count] for x in range(half)]
        mixed = []
        for j in range(half):
            total = None
            for x in range(half):
                term = xtab[pl.ds(j * half + x, 1), :] * parts[x]
                total = term if total is None else total + term
            mixed.append(total)
        return [
            jnp.concatenate([mixed[j][f * count:(f + 1) * count] for j in range(half)], axis=0)
            for f in range(3)
        ]

    slot = s * span + (t - base)

    tau = t - base
    paired = all_solve and span & (span - 1) == 0 and ns & (ns - 1) == 0

    def flipped(value, mask):
        for bit in range(mask.bit_length()):
            if mask >> bit & 1:
                value = value + (1 - 2 * (value // 2 ** bit % 2)) * 2 ** bit
        return value

    def flips():
        return sorted(((a, b) for a in range(span) for b in range(ns) if a or b), key=far_first)

    def spread(source_of, target, sem):
        def go(a, to_t, to_s):
            remote(
                source_of(pl.ds(pl.multiple_of(a * 8, 8), 8)), target.at[slot],
                sems.at[sem], sems.at[sem + 1], (to_t, to_s),
            ).start()

        if paired:
            for flip_t, flip_s in flips():
                to_tau, to_s = flipped(tau, flip_t), flipped(s, flip_s)
                go(to_tau * ns + to_s, base + to_tau, to_s)
        else:
            def body(a, carry):
                to_t, to_s = place_of(a)

                @pl.when((to_t != t) | (to_s != s))
                def _():
                    go(a, to_t, to_s)

                return carry

            lax.fori_loop(0, solvers, body, 0)

    def late(k):
        high = half * late_c
        for f, field in enumerate(transformed(early_c + k * late_c, late_c)):
            staged[k, pl.ds(pl.multiple_of(lax.rem(f + s, blocks) * high, 8), high), :] = field
        for f in range(3, blocks):
            staged[k, pl.ds(pl.multiple_of(lax.rem(f + s, blocks) * high, 8), high), :] = jnp.zeros(
                (high, width), jnp.float32
            )
        send_l[k] = jnp.transpose(staged[k])

    early_steps = early_c * 2 // BLOCK
    with jax.named_scope("steps"):
        lax.fori_loop(0, early_steps, main_step, 0)

    with jax.named_scope("fwd_a"):
        for copy in tables:
            copy.wait()
        if early_c > 0:
            together = transformed(0, early_c)
            filled = half * early_c
            per_tile = length // filled
            for i in range(tiles):
                parts = together[i * per_tile:(i + 1) * per_tile]
                if len(parts) * filled < length:
                    parts.append(jnp.zeros((length - len(parts) * filled, width), jnp.float32))
                send_a[i] = jnp.transpose(jnp.concatenate(parts, axis=0))

    hear(rounds - 1)
    if early_c > 0:
        with jax.named_scope("issue_a"):
            spread(lambda r: send_a.at[:, r], recv_a, 0)

    with jax.named_scope("steps_m"):
        lax.fori_loop(early_steps, steps, main_step, 0)

    if middles:
        with jax.named_scope("fwd_m"):
            late(0)
        with jax.named_scope("issue_m"):
            spread(lambda r: send_l.at[0, r], recv_l.at[0], 8)

    with jax.named_scope("w_final"):
        @pl.when(t > 0)
        def _():
            final.wait_recv()

    with jax.named_scope("tail"):
        step(HALO + 4 + steps * BLOCK, 2 * BLOCK)

    with jax.named_scope("fwd_b"):
        late(middles)
    with jax.named_scope("issue_b"):
        spread(lambda r: send_l.at[middles, r], recv_l.at[middles], 6)

    with jax.named_scope("sent"):
        for copy in halos:
            copy.wait_send()

        @pl.when(t < nt - 1)
        def _():
            for copy in starts:
                copy.wait_send()

        for copy in inits:
            copy.wait_send()

    def when_solver(body):
        if all_solve:
            body()
        else:
            pl.when(is_solver)(body)

    def bytes_wait(ref, count, sem):
        if count > 0:
            part = ref.at[pl.ds(0, count)]
            pltpu.make_async_copy(part, part, sem).wait()

    def forward_sent(count):
        if early_c > 0:
            bytes_wait(recv_a, count, sems.at[0])
        if middles:
            bytes_wait(recv_l.at[0], count, sems.at[8])
        bytes_wait(recv_l.at[middles], count, sems.at[6])

    def carry_copy(to_t):
        return remote(carry_out, carry_in, sems.at[4], sems.at[5], (to_t, s))

    def solve():
        at = pl.multiple_of(mine * 8, 8)
        if early_c > 0:
            recv_a[slot] = send_a[:, pl.ds(at, 8)]
        for k in range(middles + 1):
            recv_l[k, slot] = send_l[k, pl.ds(at, 8), :]
        factor = inv[pl.ds(at, 8), :]
        spectra = None
        tall = span * 8
        if early_c > 0:
            with jax.named_scope("w_recv_a"):
                bytes_wait(recv_a, span * ns - 1, sems.at[1])
            with jax.named_scope("z_a"):
                filled = half * early_c
                per_tile = length // filled
                lane = lax.broadcasted_iota(jnp.int32, (tall, length), 1) // filled
                fields = []
                for f in range(3):
                    columns = []
                    for k in range(-(-ns // per_tile)):
                        chosen = jnp.zeros((tall, length), jnp.float32)
                        for g in range(min(per_tile, ns - k * per_tile)):
                            q = k * per_tile + g
                            value = recv_a[pl.ds(q * span, span), f // per_tile].reshape(tall, length)
                            shift = (g - f % per_tile) * filled % length
                            if shift:
                                value = pltpu.roll(value, shift, 1)
                            chosen = jnp.where(lane == g, value, chosen)
                        columns.append(chosen)
                    fields.append(jnp.concatenate(columns, axis=1))
                spectra = product(halves(jnp.concatenate(fields, axis=0)), (zearly[0], zearly[1]), ((1,), (0,)))

        def late_part(k):
            high = half * late_c
            arrived = [recv_l[k, pl.ds(q * span, span)].reshape(tall, length) for q in range(ns)]
            lane = lax.broadcasted_iota(jnp.int32, (tall, length), 1) // high
            fields = []
            for f in range(3):
                columns = []
                for c in range(-(-ns // blocks)):
                    chosen = jnp.zeros((tall, length), jnp.float32)
                    for q in range(c * blocks, min(ns, (c + 1) * blocks)):
                        chosen = jnp.where(lane == (f + q) % blocks, arrived[q], chosen)
                    if f > 0:
                        chosen = pltpu.roll(chosen, length - high * f, 1)
                    columns.append(chosen)
                fields.append(jnp.concatenate(columns, axis=1))
            return product(halves(jnp.concatenate(fields, axis=0)), (zlate[k, 0], zlate[k, 1]), ((1,), (0,)))

        if middles:
            with jax.named_scope("w_recv_m"):
                bytes_wait(recv_l.at[0], span * ns - 1, sems.at[9])
            with jax.named_scope("z_m"):
                more = late_part(0)
                spectra = more if spectra is None else spectra + more
        with jax.named_scope("w_recv_b"):
            bytes_wait(recv_l.at[middles], span * ns - 1, sems.at[7])
        with jax.named_scope("solve"):
            more = late_part(middles)
            spectra = more if spectra is None else spectra + more
            height = span * 8

            if groups > 1:
                carry_in_zero = group == 0

                @pl.when(carry_in_zero)
                def _():
                    carry_in[...] = jnp.zeros(carry_in.shape, jnp.float32)

                @pl.when(group > 0)
                def _():
                    carry_copy(t).wait_recv()

                begin = carry_in[...]
            else:
                begin = jnp.zeros(factor.shape, jnp.float32)
            fields = [[], [], []]
            for n in range(span):
                part = [spectra[f * height + n * 8:f * height + n * 8 + 8] for f in range(3)]
                middle = (begin + part[0]) * factor
                finish = (middle + part[1]) * factor
                for f, value in enumerate((begin, middle, finish)):
                    fields[f].append(value)
                begin = finish + part[2]
            if groups > 1:
                carry_out[...] = begin

                @pl.when(group < groups - 1)
                def _():
                    carry_copy(t + span).start()

            whole_c = zback.shape[1] // 2
            rows_all = jnp.concatenate(
                [
                    jnp.concatenate([value[:, j * whole_c:(j + 1) * whole_c] for field in fields for value in field], axis=0)
                    for j in range(half)
                ],
                axis=0,
            )
            upper, lower = halves(rows_all)
            wide = lax.dot_general(
                jnp.concatenate([upper, lower], axis=1), zback[...], (((1,), (0,)), ((), ())),
                preferred_element_type=jnp.float32,
            )
            back = wide[:, :whole_c] + wide[:, whole_c:]
            turned = []
            for j in range(half):
                part = back[j * 3 * height:(j + 1) * 3 * height]
                turned.append(pltpu.roll(part, j * depth_c, 1) if j else part)
            lane = lax.broadcasted_iota(jnp.int32, (3 * height, length), 1) // depth_c
            for q in range(ns):
                message = turned[half - 1]
                for j in range(half - 1):
                    message = jnp.where(lane == (q + j) % ns, turned[j], message)
                for f in range(3):
                    send_2[pl.ds(q * span, span), f] = message[f * height:(f + 1) * height].reshape(span, 8, length)

        peers = span * ns

        def go(to_tau, to_s):
            remote(
                send_2.at[to_s * span + to_tau], recv_2.at[mine], sems.at[2], sems.at[3],
                (base + to_tau, to_s),
            ).start()

        with jax.named_scope("issue2"):
            if paired:
                for flip_t, flip_s in flips():
                    go(flipped(tau, flip_t), flipped(s, flip_s))
            else:
                def give(i, carry):
                    other = lax.rem(slot + i, peers)
                    go(lax.rem(other, span), other // span)
                    return carry

                lax.fori_loop(1, peers, give, 0)
        recv_2[mine] = send_2[slot]
        forward_sent(solvers - 1)
        with jax.named_scope("w_recv2"):
            bytes_wait(recv_2, solvers - 1, sems.at[3])

    when_solver(solve)
    if not all_solve:
        @pl.when(jnp.logical_not(is_solver))
        def _():
            forward_sent(solvers)
            with jax.named_scope("w_recv2"):
                bytes_wait(recv_2, solvers, sems.at[3])

    def sent():
        bytes_wait(send_2, span * ns - 1, sems.at[2])
        if groups > 1:
            @pl.when(group < groups - 1)
            def _():
                carry_copy(t).wait_send()

    when_solver(sent)


def finish(w, recv, ytab, xtab, out, returned, up, result, sems):
    _, _, interp = node_tables()
    depth, rows, cols = out.shape[2:]
    depth_c, rows_c = depth // 2, rows // 2
    half = rows_c // 2
    solvers, _, _, length = recv.shape
    count = depth_c // up.shape[0]
    s = lax.axis_index("space")
    slabs = length // depth_c
    for f in range(3):
        returned[f] = jnp.transpose(recv[:, f].reshape(solvers * 8, length))
    places = [lax.rem(s + j, slabs) * depth_c for j in range(half)]

    def give(p):
        return pltpu.make_async_copy(result.at[p], out.at[0, :, pl.ds(p * 2 * count, 2 * count)], sems.at[p])

    for p in range(up.shape[0]):
        mixed = [
            jnp.concatenate(
                [returned[f, pl.ds(pl.multiple_of(places[j] + p * count, 8), count), :] for f in range(3)], axis=0
            )
            for j in range(half)
        ]
        parts = []
        for x in range(half):
            total = None
            for j in range(half):
                term = xtab[pl.ds(j * half + x, 1), :] * mixed[j]
                total = term if total is None else total + term
            parts.append(total)
        coarse = product(halves(jnp.concatenate(parts, axis=0)), (ytab[0], ytab[1]), ((1,), (1,)))
        high = 3 * count
        for x in range(rows_c):
            part = coarse[(x % half) * high:(x % half + 1) * high, (x // half) * cols:(x // half + 1) * cols]
            for side in range(2):
                up[p, pl.ds(2 * x + side, high, stride=rows), :] = part
        for z in range(count):
            fields = [up[p, pl.ds((f * count + z) * rows, rows), :] for f in range(3)]
            for m in range(5):
                total = None
                for c in range(3):
                    if abs(interp[m][c]) < 1e-14:
                        continue
                    term = fields[c]
                    if abs(interp[m][c] - 1.0) > 1e-14:
                        term = interp[m][c] * term
                    total = term if total is None else total + term
                for side in range(2):
                    result[p, m, 2 * z + side] = w[m, HALO + 2 * (p * count + z) + side] + total
        give(p).start()
    for p in range(up.shape[0]):
        give(p).wait()


def shards(nt, ns, u_old, u_init):
    depth, rows, cols = u_init.shape
    depth_c, rows_c, cols_c = depth // 2, rows // 2, cols // 2
    half = rows_c // 2
    whole_c = depth_c * ns
    width = 2 * cols_c
    solvers = width // 8
    groups = GROUPS
    span = nt // groups
    length = -(-half * depth_c // 128) * 128
    extended = depth + 2 * HALO
    rounds = max(1, (nt - 1).bit_length())
    steps = depth // BLOCK - 2

    wide = np.repeat(hartley(cols_c), 2, axis=0)
    zero = np.zeros_like(wide)
    forth = 0.125 * np.block([[wide, zero], [zero, wide]])
    back = np.block([[wide, wide], [wide, -wide]])
    ytab = np.stack([two_parts(forth), two_parts(back)])
    wave_x = hartley(rows_c)
    xtab = np.zeros((half * half, width), np.float32)
    for j in range(half):
        for x in range(half):
            xtab[j * half + x, :cols_c] = wave_x[2 * j, x]
            xtab[j * half + x, cols_c:] = wave_x[2 * j + 1, x]
    wave_z = hartley(whole_c).reshape(ns, depth_c, whole_c)
    late_c = BLOCK
    blocks = length // (half * late_c)
    sets = -(-ns // blocks)
    middles = 1 if depth_c > 2 * late_c else 0
    early_c = depth_c - (1 + middles) * late_c
    per_tile = length // (half * early_c) if early_c else 1
    tiles = -(-3 // per_tile) if early_c else 1
    early_sets = -(-ns // per_tile)
    zearly = np.zeros((early_sets, length, half * whole_c))
    zlate = np.zeros((middles + 1, sets * blocks, half, late_c, half, whole_c))
    for j in range(half):
        for q in range(ns if early_c else 0):
            row = q % per_tile * half * early_c + j * early_c
            zearly[q // per_tile, row:row + early_c, j * whole_c:(j + 1) * whole_c] = wave_z[q, :early_c]
        for k in range(middles + 1):
            begin = early_c + k * late_c
            zlate[k, :ns, j, :, j] = wave_z[:, begin:begin + late_c]
    zearly = two_parts(zearly.reshape(early_sets * length, half * whole_c))
    if early_c == 0:
        zearly = zearly[:, :16]
    zlate = np.stack([two_parts(part.reshape(sets * length, half * whole_c)) for part in zlate])
    wave = two_parts(hartley(whole_c))
    zback = np.block([[wave[0], wave[1]], [wave[0], np.zeros_like(wave[0])]])
    angle_z = 2.0 * np.cos(2.0 * np.pi * np.arange(whole_c) / whole_c)
    angle_x = 2.0 * np.cos(2.0 * np.pi * np.arange(rows_c) / rows_c)
    angle_y = 2.0 * np.cos(2.0 * np.pi * np.arange(cols_c) / cols_c)
    eigen = 0.25 * (
        angle_x.reshape(half, 2).T[:, None, :, None] + angle_y[None, :, None, None] + angle_z - 6.0
    )
    inv = (1.0 / (1.0 - 0.5 * step_length * diffusion * eigen)).astype(np.float32)
    inv = inv.reshape(width, half * whole_c)

    f32 = jnp.float32
    bf16 = jnp.bfloat16
    arrays = (u_old, u_init, ytab, xtab, zback, zearly, zlate, inv)
    handed = pl.pallas_call(
        functools.partial(kernel, nt, ns, groups),
        out_shape=(
            jax.ShapeDtypeStruct((5, extended, rows, cols), f32),
            jax.ShapeDtypeStruct((solvers, 3, 8, length), f32),
            jax.ShapeDtypeStruct(ytab.shape[1:], bf16),
            jax.ShapeDtypeStruct(xtab.shape, f32),
        ),
        in_specs=[pl.BlockSpec(memory_space=pltpu.HBM)] * len(arrays),
        out_specs=(pl.BlockSpec(memory_space=pltpu.VMEM),) * 4,
        scratch_shapes=[
            pltpu.VMEM((5, extended, rows, cols), f32),
            pltpu.VMEM((4, extended, rows, cols), f32),
            pltpu.VMEM((4, extended, rows, cols), f32),
            pltpu.VMEM((3 * depth_c * rows, cols), f32),
            pltpu.VMEM(ytab.shape[1:], bf16),
            pltpu.VMEM(zback.shape, bf16),
            pltpu.VMEM(zearly.shape, bf16),
            pltpu.VMEM(zlate.shape, bf16),
            pltpu.VMEM(inv.shape, f32),
            pltpu.VMEM((tiles, width, length), f32),
            pltpu.VMEM((span * ns, tiles, 8, length), f32),
            pltpu.VMEM((middles + 1, length, width), f32),
            pltpu.VMEM((middles + 1, width, length), f32),
            pltpu.VMEM((middles + 1, span * ns, 8, length), f32),
            pltpu.VMEM((span * ns, 3, 8, length), f32),
            pltpu.VMEM((8, half * whole_c), f32),
            pltpu.VMEM((8, half * whole_c), f32),
            pltpu.SemaphoreType.DMA,
            pltpu.SemaphoreType.DMA((7,)),
            pltpu.SemaphoreType.DMA,
            pltpu.SemaphoreType.DMA((2,)),
            pltpu.SemaphoreType.DMA((2,)),
            pltpu.SemaphoreType.DMA((5 + steps,)),
            pltpu.SemaphoreType.DMA((5 + steps,)),
            pltpu.SemaphoreType.DMA((10,)),
            pltpu.SemaphoreType.REGULAR((rounds,)),
        ],
        compiler_params=pltpu.CompilerParams(
            collective_id=0, has_side_effects=True, vmem_limit_bytes=36000000
        ),
    )(*(pltpu.with_memory_space_constraint(a, pltpu.HBM) for a in arrays))
    return pl.pallas_call(
        finish,
        out_shape=jax.ShapeDtypeStruct((1, 5, depth, rows, cols), f32),
        in_specs=[pl.BlockSpec(memory_space=pltpu.VMEM)] * 4,
        out_specs=pl.BlockSpec(memory_space=pltpu.HBM),
        scratch_shapes=[
            pltpu.VMEM((3, length, width), f32),
            pltpu.VMEM((depth_c // 8, 3 * 8 * rows, cols), f32),
            pltpu.VMEM((depth_c // 8, 5, 16, rows, cols), f32),
            pltpu.SemaphoreType.DMA((depth_c // 8,)),
        ],
        compiler_params=pltpu.CompilerParams(vmem_limit_bytes=16000000),
    )(*handed)


def solution(mesh):
    return jax.shard_map(
        functools.partial(shards, mesh.shape["tm"], mesh.shape["space"]),
        mesh=mesh,
        in_specs=(P("tm", None, "space", None, None), P("space", None, None)),
        out_specs=P("tm", None, "space", None, None),
        check_vma=False,
    )
```

```python
import functools
import math

import jax
import jax.numpy as jnp
import numpy as np
from jax import lax
from jax.experimental import pallas as pl
from jax.experimental.pallas import tpu as pltpu
from jax.sharding import PartitionSpec as P

step_length = 0.4
diffusion = 1.0
reaction = 1.0
HALO = 5
BLOCK = 8
GROUPS = 2
MESH = pl.DeviceIdType.MESH


def basis_coefficients(nodes, chosen):
    polynomial = [1.0]
    for other, point in enumerate(nodes):
        if other == chosen:
            continue
        divisor = nodes[chosen] - point
        widened = [0.0] * (len(polynomial) + 1)
        for power, value in enumerate(polynomial):
            widened[power + 1] += value / divisor
            widened[power] -= value * point / divisor
        polynomial = widened
    return polynomial


def basis_value(nodes, chosen, where):
    result = 1.0
    for other, point in enumerate(nodes):
        if other != chosen:
            result *= (where - point) / (nodes[chosen] - point)
    return result


def node_tables():
    root = math.sqrt(3.0 / 7.0)
    fine_tau = [0.0, (1.0 - root) / 2.0, 0.5, (1.0 + root) / 2.0, 1.0]
    coarse_tau = [0.0, 0.5, 1.0]
    integ = []
    for j in range(4):
        row_values = []
        for k in range(5):
            polynomial = basis_coefficients(fine_tau, k)
            total = 0.0
            for power, value in enumerate(polynomial):
                total += (
                    value
                    * (fine_tau[j + 1] ** (power + 1) - fine_tau[j] ** (power + 1))
                    / (power + 1)
                )
            row_values.append(total)
        integ.append(row_values)
    interp = [[basis_value(coarse_tau, c, fine_tau[m]) for c in range(3)] for m in range(5)]
    spacing = [float(fine_tau[j + 1] - fine_tau[j]) for j in range(4)]
    return integ, spacing, interp


def hartley(length):
    counter = np.arange(length)
    phase = 2.0 * np.pi * (counter[:, None] * counter[None, :] % length) / length
    return (np.cos(phase) + np.sin(phase)) / math.sqrt(length)


def two_parts(table):
    upper = table.astype(jnp.bfloat16)
    lower = (table - upper.astype(np.float64)).astype(jnp.bfloat16)
    return np.stack([upper, lower])


def halves(value):
    upper = value.astype(jnp.bfloat16)
    return upper, (value - upper.astype(jnp.float32)).astype(jnp.bfloat16)


def product(a, b, dims):
    def one(x, y):
        return lax.dot_general(x, y, (dims, ((), ())), preferred_element_type=jnp.float32)

    return one(a[0], b[0]) + (one(a[0], b[1]) + one(a[1], b[0]))


def tables_of(half_tab, width, whole_c, middles, late):
    rows = 2 * width
    early = half_tab.shape[0] - 2 * rows - (middles + 1) * 2 * late

    def forth(i):
        return half_tab[pl.ds(i * rows, rows), pl.ds(0, width)]

    def back(i):
        return half_tab[pl.ds(i * rows, rows), pl.ds(width, width)]

    def z_back():
        return half_tab[pl.ds(0, 2 * whole_c), pl.ds(2 * width, 2 * whole_c)]

    def z_early(i):
        return half_tab[pl.ds(2 * rows + i * (early // 2), early // 2), :]

    def z_late(k, i):
        return half_tab[pl.ds(2 * rows + early + (2 * k + i) * late, late), :]

    return forth, back, z_back, z_early, z_late


def far_first(flip):
    hops = bin(flip[0]).count("1") + bin(flip[1] // 2).count("1")
    return -(flip[1] // 2), -hops, -flip[0]


def force(padded):
    field = padded[1:-1]
    rows, cols = field.shape[1:]
    near = padded[2:] + padded[:-2]
    near = near + (pltpu.roll(field, 1, 1) + pltpu.roll(field, rows - 1, 1))
    near = near + (pltpu.roll(field, 1, 2) + pltpu.roll(field, cols - 1, 2))
    linear = reaction - 6.0 * diffusion
    return diffusion * near + field * (linear - reaction * (field * field))


def kernel(
    nt, ns, groups,
    u_hbm, init_hbm, half_tab_hbm, full_tab_hbm,
    w, recv_2, half_tab, full_tab,
    u, corr, forces, restricted,
    send_a, recv_a, staged, send_l, recv_l, send_2, carry_out, carry_in,
    load_sem, table_sem, start_sem, early_send, edge_recv, start_recv,
    sems, known_sem,
):
    integ, spacing, _ = node_tables()
    h = step_length
    depth, rows, cols = init_hbm.shape
    depth_c, rows_c = depth // 2, rows // 2
    half = rows_c // 2
    width = staged.shape[1]
    length = send_2.shape[3]
    late_c = BLOCK
    blocks = length // (half * late_c)
    middles = 1 if depth_c > 2 * late_c else 0
    early_c = depth_c - (1 + middles) * late_c
    tiles = send_a.shape[0]
    whole_c = depth_c * ns
    extended = depth + 2 * HALO
    ytab, _, zback, zearly, zlate = tables_of(half_tab, width, whole_c, middles, -(-ns // blocks) * length)
    inv, xtab = full_tab.at[pl.ds(0, width)], full_tab.at[pl.ds(width, half * half), pl.ds(0, width)]
    solvers = width // 8
    span = nt // groups
    own = pl.ds(HALO, depth)
    t, s = lax.axis_index("tm"), lax.axis_index("space")
    group = t // span
    base = group * span
    above, below = lax.rem(s + 1, ns), lax.rem(s + ns - 1, ns)
    per = max(1, solvers // ns)
    lead = base + (span - per) // 2
    mine = (t - lead) * ns + s
    is_solver = (t >= lead) & (mine < solvers)
    all_solve = solvers == span * ns

    def place_of(a):
        return lead + a // ns, lax.rem(a, ns)

    barrier = pltpu.get_barrier_semaphore()

    def signal_along(sem, step):
        @pl.when(t + step < nt)
        def _():
            pl.semaphore_signal(sem, inc=1, device_id=(t + step, s), device_id_type=MESH)

        @pl.when(t >= step)
        def _():
            pl.semaphore_signal(sem, inc=1, device_id=(t - step, s), device_id_type=MESH)

    def sides(step):
        return jnp.where(t + step < nt, 1, 0) + jnp.where(t >= step, 1, 0)

    signal_along(barrier, 1)
    for i in range(1, ns):
        pl.semaphore_signal(
            barrier, inc=1, device_id=(t, lax.rem(s + i, ns)), device_id_type=MESH
        )
    load = pltpu.make_async_copy(u_hbm.at[0], u.at[:, own], load_sem)
    load.start()
    tables = [
        pltpu.make_async_copy(half_tab_hbm, half_tab, table_sem.at[0]),
        pltpu.make_async_copy(full_tab_hbm, full_tab, table_sem.at[1]),
    ]
    for copy in tables:
        copy.start()
    local_start = pltpu.make_async_copy(init_hbm, w.at[0, own], start_sem)

    @pl.when(t == 0)
    def _():
        local_start.start()

    with jax.named_scope("barrier"):
        pl.semaphore_wait(barrier, ns - 1 + sides(1))

    lows, highs = pl.ds(0, HALO), pl.ds(HALO + depth, HALO)
    first, last = pl.ds(0, HALO), pl.ds(depth - HALO, HALO)

    def remote(source, target, send, recv, place):
        return pltpu.make_async_remote_copy(
            src_ref=source, dst_ref=target, send_sem=send, recv_sem=recv,
            device_id=place, device_id_type=MESH,
        )

    after = jnp.minimum(t + 1, nt - 1)
    node = u_hbm.at[0, 4]
    steps = depth // BLOCK - 2
    doubles = early_c // BLOCK
    singles = steps - 2 * doubles

    def start_piece(sem, begin, size):
        return remote(
            node.at[pl.ds(begin, size)], w.at[0, pl.ds(HALO + begin, size)],
            early_send, sem, (after, s),
        )

    def inner(i, size, base_chunk):
        return start_piece(start_recv.at[base_chunk + i], HALO + (2 * doubles if base_chunk else 0) * BLOCK + i * size, size)

    def planes_wait(count, sem):
        whole = next(k for k in range(1, 6) if count % k == 0 and count // k <= extended)
        part = u.at[pl.ds(0, whole), pl.ds(0, count // whole)]
        pltpu.make_async_copy(part, part, sem).wait()

    start_edges = [start_piece(edge_recv.at[0], 0, HALO), start_piece(edge_recv.at[0], depth - HALO, HALO)]
    final = start_piece(start_recv.at[doubles + singles], HALO + steps * BLOCK, depth - 2 * HALO - steps * BLOCK)
    starts = start_edges + [inner(i, 2 * BLOCK, 0) for i in range(doubles)]
    starts += [inner(i, BLOCK, doubles) for i in range(singles)] + [final]

    def edges(source, shift):
        return [
            remote(
                source.at[pl.ds(shift + depth - HALO, HALO)], w.at[0, lows],
                early_send, edge_recv.at[1], (t, above),
            ),
            remote(
                source.at[pl.ds(shift, HALO)], w.at[0, highs],
                early_send, edge_recv.at[1], (t, below),
            ),
        ]

    inits, passed = edges(init_hbm, 0), edges(w.at[0], HALO)
    halos = [
        remote(u_hbm.at[0, :, last], u.at[:, lows], early_send, load_sem, (t, above)),
        remote(u_hbm.at[0, :, first], u.at[:, highs], early_send, load_sem, (t, below)),
    ]

    @pl.when(t < nt - 1)
    def _():
        for copy in starts:
            copy.start()

    for copy in halos:
        copy.start()

    @pl.when(t == 0)
    def _():
        for copy in inits:
            copy.start()

    signal_along(known_sem.at[0], 1)
    rounds = known_sem.shape[0]

    def hear(i):
        pl.semaphore_wait(known_sem.at[i], sides(2 ** i))
        if i + 1 < rounds:
            signal_along(known_sem.at[i + 1], 2 ** (i + 1))

    with jax.named_scope("w_edges"):
        @pl.when(t > 0)
        def _():
            planes_wait(2 * HALO, edge_recv.at[0])
            for copy in passed:
                copy.start()

    if rounds > 1:
        hear(0)

    with jax.named_scope("w_halo"):
        pltpu.make_async_copy(u, u, load_sem).wait()

    if rounds > 2:
        hear(1)

    def fold_block(i, carry):
        z = 1 + i * BLOCK
        parts = [force(u[k, pl.ds(z - 1, BLOCK + 2)]) for k in range(5)]
        for j in range(4):
            total = None
            for k in range(5):
                weight = h * integ[j][k] - (h * spacing[j] if j == k else 0.0)
                term = weight * parts[k]
                total = term if total is None else total + term
            corr[j, pl.ds(z, BLOCK)] = total
        return carry

    with jax.named_scope("fold"):
        lax.fori_loop(0, (depth + 2 * HALO - 2) // BLOCK, fold_block, 0)

    for i in range(2, rounds - 1):
        hear(i)

    @pl.when(t == 0)
    def _():
        local_start.wait()

    planes_wait(2 * HALO, edge_recv.at[1])

    def advance(m, padded, here):
        now = force(padded)
        forces[m, here] = now
        result = padded[1:-1] + (h * spacing[m]) * now + corr[m, here]
        w[m + 1, here] = result
        return result

    plane = rows * depth_c

    def step(begin, count):
        reached = None
        for m in range(5):
            at = begin - m
            if m == 0:
                padded = w[0, pl.ds(at - 1, count + 2)]
            else:
                padded = jnp.concatenate([w[m, pl.ds(at - 1, 2)], reached], axis=0)
            if m < 4:
                reached = advance(m, padded, pl.ds(at, count))
        here = pl.ds(at, count)
        now, end = force(padded), padded[1:-1]
        middle = w[2, here]
        olds = [forces[m, here] for m in range(4)] + [now]
        outs = []
        for a in range(2):
            total = (w[0, here] - middle) if a == 0 else (middle - end)
            for m in range(5):
                total = total + (h * (integ[2 * a][m] + integ[2 * a + 1][m])) * olds[m]
            outs.append(total)
        outs.append(end - u[4, here])
        for f in range(3):
            pair = outs[f].reshape(count // 2, 2, rows, cols)
            pair = pair[:, 0] + pair[:, 1]
            to = f * plane + (at - HALO) // 2 * rows
            if not isinstance(to, int):
                to = pl.multiple_of(to, 8)
            restricted[pl.ds(to, count // 2 * rows), :] = pair.reshape(count // 2 * rows, cols)

    with jax.named_scope("prologue"):
        for m in range(4):
            count = BLOCK - 2 * m
            advance(m, w[m, pl.ds(m, count + 2)], pl.ds(1 + m, count))

    def main_steps(count, size, base_chunk):
        first_z = HALO + 4 + (2 * doubles if base_chunk else 0) * BLOCK

        def body(i, carry):
            @pl.when(t > 0)
            def _():
                inner(i, size, base_chunk).wait_recv()

            step(first_z + i * size, size)
            return carry

        lax.fori_loop(0, count, body, 0)

    def transformed(begin, count):
        slabs = []
        for x in range(rows_c):
            fields = []
            for f in range(3):
                at = f * plane + begin * rows + 2 * x
                even = restricted[pl.ds(at, count, stride=rows), :]
                odd = restricted[pl.ds(at + 1, count, stride=rows), :]
                fields.append(even + odd)
            slabs.append(jnp.concatenate(fields, axis=0))
        pairs = [
            jnp.concatenate([slabs[x] + slabs[x + half], slabs[x] - slabs[x + half]], axis=1)
            for x in range(half)
        ]
        turned = product(halves(jnp.concatenate(pairs, axis=0)), (ytab(0), ytab(1)), ((1,), (0,)))
        parts = [turned[x * 3 * count:(x + 1) * 3 * count] for x in range(half)]
        mixed = []
        for j in range(half):
            total = None
            for x in range(half):
                term = xtab[pl.ds(j * half + x, 1), :] * parts[x]
                total = term if total is None else total + term
            mixed.append(total)
        return [
            jnp.concatenate([mixed[j][f * count:(f + 1) * count] for j in range(half)], axis=0)
            for f in range(3)
        ]

    slot = s * span + (t - base)

    tau = t - base
    paired = all_solve and span & (span - 1) == 0 and ns & (ns - 1) == 0

    def flipped(value, mask):
        for bit in range(mask.bit_length()):
            if mask >> bit & 1:
                value = value + (1 - 2 * (value // 2 ** bit % 2)) * 2 ** bit
        return value

    def flips():
        return sorted(((a, b) for a in range(span) for b in range(ns) if a or b), key=far_first)

    def spread(source_of, target, sem):
        def go(a, to_t, to_s):
            remote(
                source_of(pl.ds(pl.multiple_of(a * 8, 8), 8)), target.at[slot],
                sems.at[0], sems.at[sem], (to_t, to_s),
            ).start()

        if paired:
            for flip_t, flip_s in flips():
                to_tau, to_s = flipped(tau, flip_t), flipped(s, flip_s)
                go(to_tau * ns + to_s, base + to_tau, to_s)
        else:
            def body(a, carry):
                to_t, to_s = place_of(a)

                @pl.when((to_t != t) | (to_s != s))
                def _():
                    go(a, to_t, to_s)

                return carry

            lax.fori_loop(0, solvers, body, 0)

    def late(k):
        high = half * late_c
        for f, field in enumerate(transformed(early_c + k * late_c, late_c)):
            staged[k, pl.ds(pl.multiple_of(lax.rem(f + s, blocks) * high, 8), high), :] = field
        for f in range(3, blocks):
            staged[k, pl.ds(pl.multiple_of(lax.rem(f + s, blocks) * high, 8), high), :] = jnp.zeros(
                (high, width), jnp.float32
            )
        send_l[k] = jnp.transpose(staged[k])

    with jax.named_scope("steps"):
        main_steps(doubles, 2 * BLOCK, 0)

    with jax.named_scope("fwd_a"):
        for copy in tables:
            copy.wait()
        if early_c > 0:
            together = transformed(0, early_c)
            filled = half * early_c
            per_tile = length // filled
            for i in range(tiles):
                parts = together[i * per_tile:(i + 1) * per_tile]
                if len(parts) * filled < length:
                    parts.append(jnp.zeros((length - len(parts) * filled, width), jnp.float32))
                send_a[i] = jnp.transpose(jnp.concatenate(parts, axis=0))

    hear(rounds - 1)
    if early_c > 0:
        with jax.named_scope("issue_a"):
            spread(lambda r: send_a.at[:, r], recv_a, 1)

    with jax.named_scope("steps_m"):
        main_steps(singles, BLOCK, doubles)

    if middles:
        with jax.named_scope("fwd_m"):
            late(0)
        with jax.named_scope("issue_m"):
            spread(lambda r: send_l.at[0, r], recv_l.at[0], 6)

    with jax.named_scope("w_final"):
        @pl.when(t > 0)
        def _():
            final.wait_recv()

    with jax.named_scope("tail"):
        step(HALO + 4 + steps * BLOCK, 2 * BLOCK)

    with jax.named_scope("fwd_b"):
        late(middles)
    with jax.named_scope("issue_b"):
        spread(lambda r: send_l.at[middles, r], recv_l.at[middles], 7)

    with jax.named_scope("sent"):
        @pl.when(t < nt - 1)
        def _():
            planes_wait(12 * HALO + depth, early_send)

        @pl.when(t == nt - 1)
        def _():
            planes_wait(12 * HALO, early_send)

    def when_solver(body):
        if all_solve:
            body()
        else:
            pl.when(is_solver)(body)

    def bytes_wait(ref, count, sem):
        if count > 0:
            part = ref.at[pl.ds(0, count)]
            pltpu.make_async_copy(part, part, sem).wait()

    def forward_sent(count):
        units = count * ((tiles if early_c > 0 else 0) + middles + 1)
        part = restricted.at[pl.ds(0, 8 * units)]
        pltpu.make_async_copy(part, part, sems.at[0]).wait()

    def carry_copy(to_t):
        return remote(carry_out, carry_in, sems.at[4], sems.at[5], (to_t, s))

    def solve():
        at = pl.multiple_of(mine * 8, 8)
        if early_c > 0:
            recv_a[slot] = send_a[:, pl.ds(at, 8)]
        for k in range(middles + 1):
            recv_l[k, slot] = send_l[k, pl.ds(at, 8), :]
        factor = inv[pl.ds(at, 8), :]
        spectra = None
        tall = span * 8
        if early_c > 0:
            with jax.named_scope("w_recv_a"):
                bytes_wait(recv_a, span * ns - 1, sems.at[1])
            with jax.named_scope("z_a"):
                filled = half * early_c
                per_tile = length // filled
                lane = lax.broadcasted_iota(jnp.int32, (tall, length), 1) // filled
                fields = []
                for f in range(3):
                    columns = []
                    for k in range(-(-ns // per_tile)):
                        chosen = jnp.zeros((tall, length), jnp.float32)
                        for g in range(min(per_tile, ns - k * per_tile)):
                            q = k * per_tile + g
                            value = recv_a[pl.ds(q * span, span), f // per_tile].reshape(tall, length)
                            shift = (g - f % per_tile) * filled % length
                            if shift:
                                value = pltpu.roll(value, shift, 1)
                            chosen = jnp.where(lane == g, value, chosen)
                        columns.append(chosen)
                    fields.append(jnp.concatenate(columns, axis=1))
                spectra = product(halves(jnp.concatenate(fields, axis=0)), (zearly(0), zearly(1)), ((1,), (0,)))

        def late_part(k):
            high = half * late_c
            arrived = [recv_l[k, pl.ds(q * span, span)].reshape(tall, length) for q in range(ns)]
            lane = lax.broadcasted_iota(jnp.int32, (tall, length), 1) // high
            fields = []
            for f in range(3):
                columns = []
                for c in range(-(-ns // blocks)):
                    chosen = jnp.zeros((tall, length), jnp.float32)
                    for q in range(c * blocks, min(ns, (c + 1) * blocks)):
                        chosen = jnp.where(lane == (f + q) % blocks, arrived[q], chosen)
                    if f > 0:
                        chosen = pltpu.roll(chosen, length - high * f, 1)
                    columns.append(chosen)
                fields.append(jnp.concatenate(columns, axis=1))
            return product(halves(jnp.concatenate(fields, axis=0)), (zlate(k, 0), zlate(k, 1)), ((1,), (0,)))

        if middles:
            with jax.named_scope("w_recv_m"):
                bytes_wait(recv_l.at[0], span * ns - 1, sems.at[6])
            with jax.named_scope("z_m"):
                more = late_part(0)
                spectra = more if spectra is None else spectra + more
        with jax.named_scope("w_recv_b"):
            bytes_wait(recv_l.at[middles], span * ns - 1, sems.at[7])
        with jax.named_scope("solve"):
            more = late_part(middles)
            spectra = more if spectra is None else spectra + more
            height = span * 8

            if groups > 1:
                carry_in_zero = group == 0

                @pl.when(carry_in_zero)
                def _():
                    carry_in[...] = jnp.zeros(carry_in.shape, jnp.float32)

                @pl.when(group > 0)
                def _():
                    carry_copy(t).wait_recv()

                begin = carry_in[...]
            else:
                begin = jnp.zeros(factor.shape, jnp.float32)
            fields = [[], [], []]
            for n in range(span):
                part = [spectra[f * height + n * 8:f * height + n * 8 + 8] for f in range(3)]
                middle = (begin + part[0]) * factor
                finish = (middle + part[1]) * factor
                for f, value in enumerate((begin, middle, finish)):
                    fields[f].append(value)
                begin = finish + part[2]
            if groups > 1:
                carry_out[...] = begin

                @pl.when(group < groups - 1)
                def _():
                    carry_copy(t + span).start()

            rows_all = jnp.concatenate(
                [
                    jnp.concatenate([value[:, j * whole_c:(j + 1) * whole_c] for field in fields for value in field], axis=0)
                    for j in range(half)
                ],
                axis=0,
            )
            upper, lower = halves(rows_all)
            wide = lax.dot_general(
                jnp.concatenate([upper, lower], axis=1), zback(), (((1,), (0,)), ((), ())),
                preferred_element_type=jnp.float32,
            )
            back = wide[:, :whole_c] + wide[:, whole_c:]
            turned = []
            for j in range(half):
                part = back[j * 3 * height:(j + 1) * 3 * height]
                turned.append(pltpu.roll(part, j * depth_c, 1) if j else part)
            lane = lax.broadcasted_iota(jnp.int32, (3 * height, length), 1) // depth_c
            for q in range(ns):
                message = turned[half - 1]
                for j in range(half - 1):
                    message = jnp.where(lane == (q + j) % ns, turned[j], message)
                for f in range(3):
                    send_2[pl.ds(q * span, span), f] = message[f * height:(f + 1) * height].reshape(span, 8, length)

        peers = span * ns

        def go(to_tau, to_s):
            remote(
                send_2.at[to_s * span + to_tau], recv_2.at[mine], sems.at[2], sems.at[3],
                (base + to_tau, to_s),
            ).start()

        with jax.named_scope("issue2"):
            if paired:
                for flip_t, flip_s in flips():
                    go(flipped(tau, flip_t), flipped(s, flip_s))
            else:
                def give(i, carry):
                    other = lax.rem(slot + i, peers)
                    go(lax.rem(other, span), other // span)
                    return carry

                lax.fori_loop(1, peers, give, 0)
        recv_2[mine] = send_2[slot]
        forward_sent(solvers - 1)
        with jax.named_scope("w_recv2"):
            bytes_wait(recv_2, solvers - 1, sems.at[3])

    when_solver(solve)
    if not all_solve:
        @pl.when(jnp.logical_not(is_solver))
        def _():
            forward_sent(solvers)
            with jax.named_scope("w_recv2"):
                bytes_wait(recv_2, solvers, sems.at[3])

    def sent():
        bytes_wait(send_2, span * ns - 1, sems.at[2])
        if groups > 1:
            @pl.when(group < groups - 1)
            def _():
                carry_copy(t).wait_send()

    when_solver(sent)


def finish(w, recv, half_tab, full_tab, out, returned, up, result, sems):
    _, _, interp = node_tables()
    depth, rows, cols = out.shape[2:]
    depth_c, rows_c = depth // 2, rows // 2
    half = rows_c // 2
    solvers, _, _, length = recv.shape
    count = depth_c // up.shape[0]
    s = lax.axis_index("space")
    slabs = length // depth_c
    width = solvers * 8
    _, ytab, _, _, _ = tables_of(half_tab, width, length, 0, 0)
    xtab = full_tab.at[pl.ds(width, half * half), pl.ds(0, width)]
    for f in range(3):
        returned[f] = jnp.transpose(recv[:, f].reshape(solvers * 8, length))
    places = [lax.rem(s + j, slabs) * depth_c for j in range(half)]

    def give(p):
        return pltpu.make_async_copy(result.at[p], out.at[0, :, pl.ds(p * 2 * count, 2 * count)], sems.at[p])

    for p in range(up.shape[0]):
        mixed = [
            jnp.concatenate(
                [returned[f, pl.ds(pl.multiple_of(places[j] + p * count, 8), count), :] for f in range(3)], axis=0
            )
            for j in range(half)
        ]
        parts = []
        for x in range(half):
            total = None
            for j in range(half):
                term = xtab[pl.ds(j * half + x, 1), :] * mixed[j]
                total = term if total is None else total + term
            parts.append(total)
        coarse = product(halves(jnp.concatenate(parts, axis=0)), (ytab(0), ytab(1)), ((1,), (1,)))
        high = 3 * count
        for x in range(rows_c):
            part = coarse[(x % half) * high:(x % half + 1) * high, (x // half) * cols:(x // half + 1) * cols]
            for side in range(2):
                up[p, pl.ds(2 * x + side, high, stride=rows), :] = part
        for z in range(count):
            fields = [up[p, pl.ds((f * count + z) * rows, rows), :] for f in range(3)]
            for m in range(5):
                total = None
                for c in range(3):
                    if abs(interp[m][c]) < 1e-14:
                        continue
                    term = fields[c]
                    if abs(interp[m][c] - 1.0) > 1e-14:
                        term = interp[m][c] * term
                    total = term if total is None else total + term
                for side in range(2):
                    result[p, m, 2 * z + side] = w[m, HALO + 2 * (p * count + z) + side] + total
        give(p).start()
    for p in range(up.shape[0]):
        give(p).wait()


def shards(nt, ns, u_old, u_init):
    depth, rows, cols = u_init.shape
    depth_c, rows_c, cols_c = depth // 2, rows // 2, cols // 2
    half = rows_c // 2
    whole_c = depth_c * ns
    width = 2 * cols_c
    solvers = width // 8
    groups = GROUPS
    span = nt // groups
    length = -(-half * depth_c // 128) * 128
    extended = depth + 2 * HALO
    rounds = max(1, (nt - 1).bit_length())
    steps = depth // BLOCK - 2

    wide = np.repeat(hartley(cols_c), 2, axis=0)
    zero = np.zeros_like(wide)
    forth = 0.125 * np.block([[wide, zero], [zero, wide]])
    back = np.block([[wide, wide], [wide, -wide]])
    ytab = np.stack([two_parts(forth), two_parts(back)])
    wave_x = hartley(rows_c)
    xtab = np.zeros((half * half, width), np.float32)
    for j in range(half):
        for x in range(half):
            xtab[j * half + x, :cols_c] = wave_x[2 * j, x]
            xtab[j * half + x, cols_c:] = wave_x[2 * j + 1, x]
    wave_z = hartley(whole_c).reshape(ns, depth_c, whole_c)
    late_c = BLOCK
    blocks = length // (half * late_c)
    sets = -(-ns // blocks)
    middles = 1 if depth_c > 2 * late_c else 0
    early_c = depth_c - (1 + middles) * late_c
    per_tile = length // (half * early_c) if early_c else 1
    tiles = -(-3 // per_tile) if early_c else 1
    early_sets = -(-ns // per_tile) if early_c else 0
    zearly = np.zeros((early_sets, length, half * whole_c))
    zlate = np.zeros((middles + 1, sets * blocks, half, late_c, half, whole_c))
    for j in range(half):
        for q in range(ns if early_c else 0):
            row = q % per_tile * half * early_c + j * early_c
            zearly[q // per_tile, row:row + early_c, j * whole_c:(j + 1) * whole_c] = wave_z[q, :early_c]
        for k in range(middles + 1):
            begin = early_c + k * late_c
            zlate[k, :ns, j, :, j] = wave_z[:, begin:begin + late_c]
    zearly = two_parts(zearly.reshape(early_sets * length, half * whole_c))
    zlate = np.stack([two_parts(part.reshape(sets * length, half * whole_c)) for part in zlate])
    wave = two_parts(hartley(whole_c))
    zback = np.block([[wave[0], wave[1]], [wave[0], np.zeros_like(wave[0])]])
    angle_z = 2.0 * np.cos(2.0 * np.pi * np.arange(whole_c) / whole_c)
    angle_x = 2.0 * np.cos(2.0 * np.pi * np.arange(rows_c) / rows_c)
    angle_y = 2.0 * np.cos(2.0 * np.pi * np.arange(cols_c) / cols_c)
    eigen = 0.25 * (
        angle_x.reshape(half, 2).T[:, None, :, None] + angle_y[None, :, None, None] + angle_z - 6.0
    )
    inv = (1.0 / (1.0 - 0.5 * step_length * diffusion * eigen)).astype(np.float32)
    inv = inv.reshape(width, half * whole_c)

    total = half * whole_c
    misc = np.zeros((4 * width, total), jnp.bfloat16)
    misc[:, :width] = ytab[0].reshape(4 * width, width)
    misc[:, width:2 * width] = ytab[1].reshape(4 * width, width)
    misc[:2 * whole_c, 2 * width:2 * width + 2 * whole_c] = zback
    half_tab = np.concatenate([misc, zearly.reshape(-1, total), zlate.reshape(-1, total)], axis=0)
    full_tab = np.zeros((width + half * half, total), np.float32)
    full_tab[:width], full_tab[width:, :width] = inv, xtab
    f32 = jnp.float32
    bf16 = jnp.bfloat16
    arrays = (u_old, u_init, half_tab, full_tab)
    handed = pl.pallas_call(
        functools.partial(kernel, nt, ns, groups),
        out_shape=(
            jax.ShapeDtypeStruct((5, extended, rows, cols), f32),
            jax.ShapeDtypeStruct((solvers, 3, 8, length), f32),
            jax.ShapeDtypeStruct(half_tab.shape, bf16),
            jax.ShapeDtypeStruct(full_tab.shape, f32),
        ),
        in_specs=[pl.BlockSpec(memory_space=pltpu.HBM)] * len(arrays),
        out_specs=(pl.BlockSpec(memory_space=pltpu.VMEM),) * 4,
        scratch_shapes=[
            pltpu.VMEM((5, extended, rows, cols), f32),
            pltpu.VMEM((4, extended, rows, cols), f32),
            pltpu.VMEM((4, extended, rows, cols), f32),
            pltpu.VMEM((3 * depth_c * rows, cols), f32),
            pltpu.VMEM((tiles, width, length), f32),
            pltpu.VMEM((span * ns, tiles, 8, length), f32),
            pltpu.VMEM((middles + 1, length, width), f32),
            pltpu.VMEM((middles + 1, width, length), f32),
            pltpu.VMEM((middles + 1, span * ns, 8, length), f32),
            pltpu.VMEM((span * ns, 3, 8, length), f32),
            pltpu.VMEM((8, half * whole_c), f32),
            pltpu.VMEM((8, half * whole_c), f32),
            pltpu.SemaphoreType.DMA,
            pltpu.SemaphoreType.DMA((2,)),
            pltpu.SemaphoreType.DMA,
            pltpu.SemaphoreType.DMA,
            pltpu.SemaphoreType.DMA((2,)),
            pltpu.SemaphoreType.DMA((steps - early_c // BLOCK + 1,)),
            pltpu.SemaphoreType.DMA((8,)),
            pltpu.SemaphoreType.REGULAR((rounds,)),
        ],
        compiler_params=pltpu.CompilerParams(
            collective_id=0, has_side_effects=True, vmem_limit_bytes=36000000
        ),
    )(*(pltpu.with_memory_space_constraint(a, pltpu.HBM) for a in arrays))
    return pl.pallas_call(
        finish,
        out_shape=jax.ShapeDtypeStruct((1, 5, depth, rows, cols), f32),
        in_specs=[pl.BlockSpec(memory_space=pltpu.VMEM)] * 4,
        out_specs=pl.BlockSpec(memory_space=pltpu.HBM),
        scratch_shapes=[
            pltpu.VMEM((3, length, width), f32),
            pltpu.VMEM((depth_c // 8, 3 * 8 * rows, cols), f32),
            pltpu.VMEM((depth_c // 8, 5, 16, rows, cols), f32),
            pltpu.SemaphoreType.DMA((depth_c // 8,)),
        ],
        compiler_params=pltpu.CompilerParams(vmem_limit_bytes=16000000),
    )(*handed)


def solution(mesh):
    return jax.shard_map(
        functools.partial(shards, mesh.shape["tm"], mesh.shape["space"]),
        mesh=mesh,
        in_specs=(P("tm", None, "space", None, None), P("space", None, None)),
        out_specs=P("tm", None, "space", None, None),
        check_vma=False,
    )
```

```python
import functools
import math

import jax
import jax.numpy as jnp
import numpy as np
from jax import lax
from jax.experimental import pallas as pl
from jax.experimental.pallas import tpu as pltpu
from jax.sharding import PartitionSpec as P

step_length = 0.4
diffusion = 1.0
reaction = 1.0
HALO = 5
BLOCK = 8
AHEAD = 2
RELAYS = 3
GROUPS = 2
MESH = pl.DeviceIdType.MESH


def basis_coefficients(nodes, chosen):
    polynomial = [1.0]
    for other, point in enumerate(nodes):
        if other == chosen:
            continue
        divisor = nodes[chosen] - point
        widened = [0.0] * (len(polynomial) + 1)
        for power, value in enumerate(polynomial):
            widened[power + 1] += value / divisor
            widened[power] -= value * point / divisor
        polynomial = widened
    return polynomial


def basis_value(nodes, chosen, where):
    result = 1.0
    for other, point in enumerate(nodes):
        if other != chosen:
            result *= (where - point) / (nodes[chosen] - point)
    return result


def node_tables():
    root = math.sqrt(3.0 / 7.0)
    fine_tau = [0.0, (1.0 - root) / 2.0, 0.5, (1.0 + root) / 2.0, 1.0]
    coarse_tau = [0.0, 0.5, 1.0]
    integ = []
    for j in range(4):
        row_values = []
        for k in range(5):
            polynomial = basis_coefficients(fine_tau, k)
            total = 0.0
            for power, value in enumerate(polynomial):
                total += (
                    value
                    * (fine_tau[j + 1] ** (power + 1) - fine_tau[j] ** (power + 1))
                    / (power + 1)
                )
            row_values.append(total)
        integ.append(row_values)
    interp = [[basis_value(coarse_tau, c, fine_tau[m]) for c in range(3)] for m in range(5)]
    spacing = [float(fine_tau[j + 1] - fine_tau[j]) for j in range(4)]
    return integ, spacing, interp


def hartley(length):
    counter = np.arange(length)
    phase = 2.0 * np.pi * (counter[:, None] * counter[None, :] % length) / length
    return (np.cos(phase) + np.sin(phase)) / math.sqrt(length)


def two_parts(table):
    upper = table.astype(jnp.bfloat16)
    lower = (table - upper.astype(np.float64)).astype(jnp.bfloat16)
    return np.stack([upper, lower])


def halves(value):
    upper = value.astype(jnp.bfloat16)
    return upper, (value - upper.astype(jnp.float32)).astype(jnp.bfloat16)


def product(a, b, dims):
    def one(x, y):
        return lax.dot_general(x, y, (dims, ((), ())), preferred_element_type=jnp.float32)

    return one(a[0], b[0]) + (one(a[0], b[1]) + one(a[1], b[0]))


def tables_of(half_tab, width, whole_c, middles, late):
    rows = 2 * width
    early = half_tab.shape[0] - 2 * rows - (middles + 1) * 2 * late

    def forth(i):
        return half_tab[pl.ds(i * rows, rows), pl.ds(0, width)]

    def back(i):
        return half_tab[pl.ds(i * rows, rows), pl.ds(width, width)]

    def z_back():
        return half_tab[pl.ds(0, 2 * whole_c), pl.ds(2 * width, 2 * whole_c)]

    def z_early(i):
        return half_tab[pl.ds(2 * rows + i * (early // 2), early // 2), :]

    def z_late(k, i):
        return half_tab[pl.ds(2 * rows + early + (2 * k + i) * late, late), :]

    return forth, back, z_back, z_early, z_late


def far_first(flip):
    hops = bin(flip[0]).count("1") + bin(flip[1] // 2).count("1")
    return -(flip[1] // 2), -hops, -flip[0]


def force(padded):
    field = padded[1:-1]
    rows, cols = field.shape[1:]
    near = padded[2:] + padded[:-2]
    near = near + (pltpu.roll(field, 1, 1) + pltpu.roll(field, rows - 1, 1))
    near = near + (pltpu.roll(field, 1, 2) + pltpu.roll(field, cols - 1, 2))
    linear = reaction - 6.0 * diffusion
    return diffusion * near + field * (linear - reaction * (field * field))


def kernel(
    nt, ns, groups,
    u_hbm, init_hbm, half_tab_hbm, full_tab_hbm,
    w, recv_2, half_tab, full_tab,
    u, corr, forces, restricted,
    send_a, recv_a, staged, send_l, recv_l, send_2, carry_out, carry_in,
    held,
    load_sem, table_sem, start_sem, early_send, edge_recv, start_recv, relay_sems,
    sems, known_sem,
):
    integ, spacing, _ = node_tables()
    h = step_length
    depth, rows, cols = init_hbm.shape
    depth_c, rows_c = depth // 2, rows // 2
    half = rows_c // 2
    width = staged.shape[1]
    length = send_2.shape[3]
    late_c = BLOCK
    blocks = length // (half * late_c)
    middles = 1 if depth_c > 2 * late_c else 0
    early_c = depth_c - (1 + middles) * late_c
    tiles = send_a.shape[0]
    whole_c = depth_c * ns
    extended = depth + 2 * HALO
    ytab, _, zback, zearly, zlate = tables_of(half_tab, width, whole_c, middles, -(-ns // blocks) * length)
    inv, xtab = full_tab.at[pl.ds(0, width)], full_tab.at[pl.ds(width, half * half), pl.ds(0, width)]
    solvers = width // 8
    span = nt // groups
    own = pl.ds(HALO, depth)
    t, s = lax.axis_index("tm"), lax.axis_index("space")
    group = t // span
    base = group * span
    above, below = lax.rem(s + 1, ns), lax.rem(s + ns - 1, ns)
    per = max(1, solvers // ns)
    lead = base + (span - per) // 2
    mine = (t - lead) * ns + s
    is_solver = (t >= lead) & (mine < solvers)
    all_solve = solvers == span * ns

    def place_of(a):
        return lead + a // ns, lax.rem(a, ns)

    barrier = pltpu.get_barrier_semaphore()

    def signal_along(sem, step):
        @pl.when(t + step < nt)
        def _():
            pl.semaphore_signal(sem, inc=1, device_id=(t + step, s), device_id_type=MESH)

        @pl.when(t >= step)
        def _():
            pl.semaphore_signal(sem, inc=1, device_id=(t - step, s), device_id_type=MESH)

    def sides(step):
        return jnp.where(t + step < nt, 1, 0) + jnp.where(t >= step, 1, 0)

    signal_along(barrier, 1)
    for i in range(1, ns):
        pl.semaphore_signal(
            barrier, inc=1, device_id=(t, lax.rem(s + i, ns)), device_id_type=MESH
        )
    load = pltpu.make_async_copy(u_hbm.at[0], u.at[:, own], load_sem)
    load.start()
    tables = [
        pltpu.make_async_copy(half_tab_hbm, half_tab, table_sem.at[0]),
        pltpu.make_async_copy(full_tab_hbm, full_tab, table_sem.at[1]),
    ]
    for copy in tables:
        copy.start()
    local_start = pltpu.make_async_copy(init_hbm, w.at[0, own], start_sem)

    @pl.when(t == 0)
    def _():
        local_start.start()

    with jax.named_scope("barrier"):
        pl.semaphore_wait(barrier, ns - 1 + sides(1))

    lows, highs = pl.ds(0, HALO), pl.ds(HALO + depth, HALO)
    first, last = pl.ds(0, HALO), pl.ds(depth - HALO, HALO)

    def remote(source, target, send, recv, place):
        return pltpu.make_async_remote_copy(
            src_ref=source, dst_ref=target, send_sem=send, recv_sem=recv,
            device_id=place, device_id_type=MESH,
        )

    after = jnp.minimum(t + 1, nt - 1)
    node = u_hbm.at[0, 4]
    steps = depth // BLOCK - 2
    doubles = early_c // BLOCK
    chunks = [(HALO + i * 2 * BLOCK, 2 * BLOCK) for i in range(doubles - 1)]
    singles = steps - 2 * len(chunks)
    chunks += [(HALO + (steps - singles + i) * BLOCK, BLOCK) for i in range(singles)]
    chunks.append((HALO + steps * BLOCK, depth - 2 * HALO - steps * BLOCK))
    relays = min(held.shape[0], max(0, singles - 1)) if nt > 4 else 0
    relayed = len(chunks) - 1 - relays

    def relays_of(to):
        return jnp.where(to == 1, relays, 0)

    def start_piece(sem, begin, size):
        return remote(
            node.at[pl.ds(begin, size)], w.at[0, pl.ds(HALO + begin, size)],
            early_send, sem, (after, s),
        )

    def chunk(i):
        return start_piece(start_recv.at[i], *chunks[i])

    def planes_wait(count, sem):
        whole = next(k for k in range(1, 6) if count % k == 0 and count // k <= extended)
        part = u.at[pl.ds(0, whole), pl.ds(0, count // whole)]
        pltpu.make_async_copy(part, part, sem).wait()

    start_edges = [start_piece(edge_recv.at[0], 0, HALO), start_piece(edge_recv.at[0], depth - HALO, HALO)]

    def edges(source, shift):
        return [
            remote(
                source.at[pl.ds(shift + depth - HALO, HALO)], w.at[0, lows],
                early_send, edge_recv.at[1], (t, above),
            ),
            remote(
                source.at[pl.ds(shift, HALO)], w.at[0, highs],
                early_send, edge_recv.at[1], (t, below),
            ),
        ]

    inits, passed = edges(init_hbm, 0), edges(w.at[0], HALO)
    halos = [
        remote(u_hbm.at[0, :, last], u.at[:, lows], early_send, load_sem, (t, above)),
        remote(u_hbm.at[0, :, first], u.at[:, highs], early_send, load_sem, (t, below)),
    ]

    mine_relayed, theirs_relayed = relays_of(t), relays_of(t + 1)

    @pl.when(t < nt - 1)
    def _():
        for copy in start_edges:
            copy.start()
        for i in range(len(chunks)):
            k = i - relayed
            if 0 <= k < relays:
                @pl.when(mine_relayed >= relays - k)
                def _(i=i, k=k):
                    begin, size = chunks[i]
                    remote(
                        node.at[pl.ds(begin, size)], held.at[k], early_send, relay_sems.at[0], (t - 1, s)
                    ).start()

                @pl.when(mine_relayed < relays - k)
                def _(i=i):
                    chunk(i).start()
            else:
                chunk(i).start()

    for copy in halos:
        copy.start()

    @pl.when(t == 0)
    def _():
        for copy in inits:
            copy.start()

    signal_along(known_sem.at[0], 1)
    rounds = known_sem.shape[0]

    def hear(i):
        pl.semaphore_wait(known_sem.at[i], sides(2 ** i))
        if i + 1 < rounds:
            signal_along(known_sem.at[i + 1], 2 ** (i + 1))

    with jax.named_scope("w_edges"):
        @pl.when(t > 0)
        def _():
            planes_wait(2 * HALO, edge_recv.at[0])
            for copy in passed:
                copy.start()

    if rounds > 1:
        hear(0)

    with jax.named_scope("w_halo"):
        pltpu.make_async_copy(u, u, load_sem).wait()

    if rounds > 2:
        hear(1)
    for count in range(1, relays + 1):
        @pl.when(theirs_relayed == count)
        def _(count=count):
            planes_wait(count * BLOCK, relay_sems.at[0])
            for k in range(relays - count, relays):
                begin, size = chunks[relayed + k]
                remote(
                    held.at[k], w.at[0, pl.ds(HALO + begin, size)], relay_sems.at[1],
                    start_recv.at[relayed + k], (t + 2, s),
                ).start()

    def fold_block(i, carry):
        z = 1 + i * BLOCK
        parts = [force(u[k, pl.ds(z - 1, BLOCK + 2)]) for k in range(5)]
        for j in range(4):
            total = None
            for k in range(5):
                weight = h * integ[j][k] - (h * spacing[j] if j == k else 0.0)
                term = weight * parts[k]
                total = term if total is None else total + term
            corr[j, pl.ds(z, BLOCK)] = total
        return carry

    with jax.named_scope("fold"):
        lax.fori_loop(0, (depth + 2 * HALO - 2) // BLOCK, fold_block, 0)

    for i in range(2, rounds - 1):
        hear(i)

    @pl.when(t == 0)
    def _():
        local_start.wait()

    planes_wait(2 * HALO, edge_recv.at[1])

    def advance(m, padded, here):
        now = force(padded)
        forces[m, here] = now
        result = padded[1:-1] + (h * spacing[m]) * now + corr[m, here]
        w[m + 1, here] = result
        return result

    plane = rows * depth_c

    def step(begin, count):
        reached = None
        for m in range(5):
            at = begin - m
            if m == 0:
                padded = w[0, pl.ds(at - 1, count + 2)]
            else:
                padded = jnp.concatenate([w[m, pl.ds(at - 1, 2)], reached], axis=0)
            if m < 4:
                reached = advance(m, padded, pl.ds(at, count))
        here = pl.ds(at, count)
        now, end = force(padded), padded[1:-1]
        middle = w[2, here]
        olds = [forces[m, here] for m in range(4)] + [now]
        outs = []
        for a in range(2):
            total = (w[0, here] - middle) if a == 0 else (middle - end)
            for m in range(5):
                total = total + (h * (integ[2 * a][m] + integ[2 * a + 1][m])) * olds[m]
            outs.append(total)
        outs.append(end - u[4, here])
        for f in range(3):
            pair = outs[f].reshape(count // 2, 2, rows, cols)
            pair = pair[:, 0] + pair[:, 1]
            to = f * plane + (at - HALO) // 2 * rows
            if not isinstance(to, int):
                to = pl.multiple_of(to, 8)
            restricted[pl.ds(to, count // 2 * rows), :] = pair.reshape(count // 2 * rows, cols)

    with jax.named_scope("prologue"):
        for m in range(4):
            count = BLOCK - 2 * m
            advance(m, w[m, pl.ds(m, count + 2)], pl.ds(1 + m, count))

    def main_step(begin, size):
        @pl.when(t > 0)
        def _():
            for i, (first_z, count) in enumerate(chunks):
                if begin <= first_z and first_z + count <= begin + size:
                    chunk(i).wait_recv()

        step(begin + 4, size)

    def transformed(begin, count):
        slabs = []
        for x in range(rows_c):
            fields = []
            for f in range(3):
                at = f * plane + begin * rows + 2 * x
                even = restricted[pl.ds(at, count, stride=rows), :]
                odd = restricted[pl.ds(at + 1, count, stride=rows), :]
                fields.append(even + odd)
            slabs.append(jnp.concatenate(fields, axis=0))
        pairs = [
            jnp.concatenate([slabs[x] + slabs[x + half], slabs[x] - slabs[x + half]], axis=1)
            for x in range(half)
        ]
        turned = product(halves(jnp.concatenate(pairs, axis=0)), (ytab(0), ytab(1)), ((1,), (0,)))
        parts = [turned[x * 3 * count:(x + 1) * 3 * count] for x in range(half)]
        mixed = []
        for j in range(half):
            total = None
            for x in range(half):
                term = xtab[pl.ds(j * half + x, 1), :] * parts[x]
                total = term if total is None else total + term
            mixed.append(total)
        return [
            jnp.concatenate([mixed[j][f * count:(f + 1) * count] for j in range(half)], axis=0)
            for f in range(3)
        ]

    slot = s * span + (t - base)

    tau = t - base
    paired = all_solve and span & (span - 1) == 0 and ns & (ns - 1) == 0

    def flipped(value, mask):
        for bit in range(mask.bit_length()):
            if mask >> bit & 1:
                value = value + (1 - 2 * (value // 2 ** bit % 2)) * 2 ** bit
        return value

    def flips():
        return sorted(((a, b) for a in range(span) for b in range(ns) if a or b), key=far_first)

    def spread(source_of, target, sem):
        def go(a, to_t, to_s):
            remote(
                source_of(pl.ds(pl.multiple_of(a * 8, 8), 8)), target.at[slot],
                sems.at[0], sems.at[sem], (to_t, to_s),
            ).start()

        if paired:
            for flip_t, flip_s in flips():
                to_tau, to_s = flipped(tau, flip_t), flipped(s, flip_s)
                go(to_tau * ns + to_s, base + to_tau, to_s)
        else:
            def body(a, carry):
                to_t, to_s = place_of(a)

                @pl.when((to_t != t) | (to_s != s))
                def _():
                    go(a, to_t, to_s)

                return carry

            lax.fori_loop(0, solvers, body, 0)

    def late(k):
        high = half * late_c
        for f, field in enumerate(transformed(early_c + k * late_c, late_c)):
            staged[k, pl.ds(pl.multiple_of(lax.rem(f + s, blocks) * high, 8), high), :] = field
        for f in range(3, blocks):
            staged[k, pl.ds(pl.multiple_of(lax.rem(f + s, blocks) * high, 8), high), :] = jnp.zeros(
                (high, width), jnp.float32
            )
        send_l[k] = jnp.transpose(staged[k])

    with jax.named_scope("steps"):
        for i in range(doubles):
            main_step(HALO + i * 2 * BLOCK, 2 * BLOCK)

    with jax.named_scope("fwd_a"):
        for copy in tables:
            copy.wait()
        if early_c > 0:
            together = transformed(0, early_c)
            filled = half * early_c
            per_tile = length // filled
            for i in range(tiles):
                parts = together[i * per_tile:(i + 1) * per_tile]
                if len(parts) * filled < length:
                    parts.append(jnp.zeros((length - len(parts) * filled, width), jnp.float32))
                send_a[i] = jnp.transpose(jnp.concatenate(parts, axis=0))

    hear(rounds - 1)
    def issue_early():
        spread(lambda r: send_a.at[:, r], recv_a, 1)

    if early_c > 0:
        with jax.named_scope("issue_a"):
            pl.when(t > 0)(issue_early)

    with jax.named_scope("steps_m"):
        for i in range(2 * doubles, steps):
            main_step(HALO + i * BLOCK, BLOCK)

    if middles:
        with jax.named_scope("fwd_m"):
            late(0)
        if early_c > 0:
            pl.when(t == 0)(issue_early)
        with jax.named_scope("issue_m"):
            spread(lambda r: send_l.at[0, r], recv_l.at[0], 6)

    with jax.named_scope("w_final"):
        @pl.when(t > 0)
        def _():
            chunk(len(chunks) - 1).wait_recv()

    with jax.named_scope("tail"):
        step(HALO + 4 + steps * BLOCK, 2 * BLOCK)

    with jax.named_scope("fwd_b"):
        late(middles)
    with jax.named_scope("issue_b"):
        spread(lambda r: send_l.at[middles, r], recv_l.at[middles], 7)

    with jax.named_scope("sent"):
        @pl.when(t < nt - 1)
        def _():
            planes_wait(12 * HALO + depth, early_send)

        @pl.when(t == nt - 1)
        def _():
            planes_wait(12 * HALO, early_send)

        for count in range(1, relays + 1):
            @pl.when(theirs_relayed == count)
            def _(count=count):
                planes_wait(count * BLOCK, relay_sems.at[1])

    def when_solver(body):
        if all_solve:
            body()
        else:
            pl.when(is_solver)(body)

    def bytes_wait(ref, count, sem):
        if count > 0:
            part = ref.at[pl.ds(0, count)]
            pltpu.make_async_copy(part, part, sem).wait()

    def forward_sent(count):
        units = count * ((tiles if early_c > 0 else 0) + middles + 1)
        part = restricted.at[pl.ds(0, 8 * units)]
        pltpu.make_async_copy(part, part, sems.at[0]).wait()

    def carry_copy(to_t):
        return remote(carry_out, carry_in, sems.at[4], sems.at[5], (to_t, s))

    def solve():
        at = pl.multiple_of(mine * 8, 8)
        if early_c > 0:
            recv_a[slot] = send_a[:, pl.ds(at, 8)]
        for k in range(middles + 1):
            recv_l[k, slot] = send_l[k, pl.ds(at, 8), :]
        factor = inv[pl.ds(at, 8), :]
        spectra = None
        tall = span * 8
        if early_c > 0:
            with jax.named_scope("w_recv_a"):
                bytes_wait(recv_a, span * ns - 1, sems.at[1])
            with jax.named_scope("z_a"):
                filled = half * early_c
                per_tile = length // filled
                lane = lax.broadcasted_iota(jnp.int32, (tall, length), 1) // filled
                fields = []
                for f in range(3):
                    columns = []
                    for k in range(-(-ns // per_tile)):
                        chosen = jnp.zeros((tall, length), jnp.float32)
                        for g in range(min(per_tile, ns - k * per_tile)):
                            q = k * per_tile + g
                            value = recv_a[pl.ds(q * span, span), f // per_tile].reshape(tall, length)
                            shift = (g - f % per_tile) * filled % length
                            if shift:
                                value = pltpu.roll(value, shift, 1)
                            chosen = jnp.where(lane == g, value, chosen)
                        columns.append(chosen)
                    fields.append(jnp.concatenate(columns, axis=1))
                spectra = product(halves(jnp.concatenate(fields, axis=0)), (zearly(0), zearly(1)), ((1,), (0,)))

        def late_part(k):
            high = half * late_c
            arrived = [recv_l[k, pl.ds(q * span, span)].reshape(tall, length) for q in range(ns)]
            lane = lax.broadcasted_iota(jnp.int32, (tall, length), 1) // high
            fields = []
            for f in range(3):
                columns = []
                for c in range(-(-ns // blocks)):
                    chosen = jnp.zeros((tall, length), jnp.float32)
                    for q in range(c * blocks, min(ns, (c + 1) * blocks)):
                        chosen = jnp.where(lane == (f + q) % blocks, arrived[q], chosen)
                    if f > 0:
                        chosen = pltpu.roll(chosen, length - high * f, 1)
                    columns.append(chosen)
                fields.append(jnp.concatenate(columns, axis=1))
            return product(halves(jnp.concatenate(fields, axis=0)), (zlate(k, 0), zlate(k, 1)), ((1,), (0,)))

        if middles:
            with jax.named_scope("w_recv_m"):
                bytes_wait(recv_l.at[0], span * ns - 1, sems.at[6])
            with jax.named_scope("z_m"):
                more = late_part(0)
                spectra = more if spectra is None else spectra + more
        with jax.named_scope("w_recv_b"):
            bytes_wait(recv_l.at[middles], span * ns - 1, sems.at[7])
        with jax.named_scope("solve"):
            more = late_part(middles)
            spectra = more if spectra is None else spectra + more
            height = span * 8

            if groups > 1:
                carry_in_zero = group == 0

                @pl.when(carry_in_zero)
                def _():
                    carry_in[...] = jnp.zeros(carry_in.shape, jnp.float32)

                @pl.when(group > 0)
                def _():
                    carry_copy(t).wait_recv()

                begin = carry_in[...]
            else:
                begin = jnp.zeros(factor.shape, jnp.float32)
            fields = [[], [], []]
            for n in range(span):
                part = [spectra[f * height + n * 8:f * height + n * 8 + 8] for f in range(3)]
                middle = (begin + part[0]) * factor
                finish = (middle + part[1]) * factor
                for f, value in enumerate((begin, middle, finish)):
                    fields[f].append(value)
                begin = finish + part[2]
            if groups > 1:
                carry_out[...] = begin

                @pl.when(group < groups - 1)
                def _():
                    carry_copy(t + span).start()

            rows_all = jnp.concatenate(
                [
                    jnp.concatenate([value[:, j * whole_c:(j + 1) * whole_c] for field in fields for value in field], axis=0)
                    for j in range(half)
                ],
                axis=0,
            )
            upper, lower = halves(rows_all)
            wide = lax.dot_general(
                jnp.concatenate([upper, lower], axis=1), zback(), (((1,), (0,)), ((), ())),
                preferred_element_type=jnp.float32,
            )
            back = wide[:, :whole_c] + wide[:, whole_c:]
            turned = []
            for j in range(half):
                part = back[j * 3 * height:(j + 1) * 3 * height]
                turned.append(pltpu.roll(part, j * depth_c, 1) if j else part)
            lane = lax.broadcasted_iota(jnp.int32, (3 * height, length), 1) // depth_c
            for q in range(ns):
                message = turned[half - 1]
                for j in range(half - 1):
                    message = jnp.where(lane == (q + j) % ns, turned[j], message)
                for f in range(3):
                    send_2[pl.ds(q * span, span), f] = message[f * height:(f + 1) * height].reshape(span, 8, length)

        peers = span * ns

        def go(to_tau, to_s):
            remote(
                send_2.at[to_s * span + to_tau], recv_2.at[mine], sems.at[2], sems.at[3],
                (base + to_tau, to_s),
            ).start()

        with jax.named_scope("issue2"):
            if paired:
                for flip_t, flip_s in flips():
                    go(flipped(tau, flip_t), flipped(s, flip_s))
            else:
                def give(i, carry):
                    other = lax.rem(slot + i, peers)
                    go(lax.rem(other, span), other // span)
                    return carry

                lax.fori_loop(1, peers, give, 0)
        recv_2[mine] = send_2[slot]
        forward_sent(solvers - 1)
        with jax.named_scope("w_recv2"):
            bytes_wait(recv_2, solvers - 1, sems.at[3])

    when_solver(solve)
    if not all_solve:
        @pl.when(jnp.logical_not(is_solver))
        def _():
            forward_sent(solvers)
            with jax.named_scope("w_recv2"):
                bytes_wait(recv_2, solvers, sems.at[3])

    def sent():
        bytes_wait(send_2, span * ns - 1, sems.at[2])
        if groups > 1:
            @pl.when(group < groups - 1)
            def _():
                carry_copy(t).wait_send()

    when_solver(sent)


def finish(w, recv, half_tab, full_tab, out, returned, up, result, sems):
    _, _, interp = node_tables()
    depth, rows, cols = out.shape[2:]
    depth_c, rows_c = depth // 2, rows // 2
    half = rows_c // 2
    solvers, _, _, length = recv.shape
    count = depth_c // up.shape[0]
    s = lax.axis_index("space")
    slabs = length // depth_c
    width = solvers * 8
    _, ytab, _, _, _ = tables_of(half_tab, width, length, 0, 0)
    xtab = full_tab.at[pl.ds(width, half * half), pl.ds(0, width)]
    for f in range(3):
        returned[f] = jnp.transpose(recv[:, f].reshape(solvers * 8, length))
    places = [lax.rem(s + j, slabs) * depth_c for j in range(half)]

    def give(p):
        return pltpu.make_async_copy(result.at[p], out.at[0, :, pl.ds(p * 2 * count, 2 * count)], sems.at[p])

    def spread_up(p):
        mixed = [
            jnp.concatenate(
                [returned[f, pl.ds(pl.multiple_of(places[j] + p * count, 8), count), :] for f in range(3)], axis=0
            )
            for j in range(half)
        ]
        parts = []
        for x in range(half):
            total = None
            for j in range(half):
                term = xtab[pl.ds(j * half + x, 1), :] * mixed[j]
                total = term if total is None else total + term
            parts.append(total)
        coarse = product(halves(jnp.concatenate(parts, axis=0)), (ytab(0), ytab(1)), ((1,), (1,)))
        high = 3 * count
        for x in range(rows_c):
            part = coarse[(x % half) * high:(x % half + 1) * high, (x // half) * cols:(x // half + 1) * cols]
            for side in range(2):
                up[p, pl.ds(2 * x + side, high, stride=rows), :] = part

    def add(p):
        for z in range(count):
            fields = [up[p, pl.ds((f * count + z) * rows, rows), :] for f in range(3)]
            for m in range(5):
                total = None
                for c in range(3):
                    if abs(interp[m][c]) < 1e-14:
                        continue
                    term = fields[c]
                    if abs(interp[m][c] - 1.0) > 1e-14:
                        term = interp[m][c] * term
                    total = term if total is None else total + term
                for side in range(2):
                    result[p, m, 2 * z + side] = w[m, HALO + 2 * (p * count + z) + side] + total
        give(p).start()

    parts = up.shape[0]
    ahead = min(AHEAD, parts)
    for p in range(ahead):
        spread_up(p)
    for p in range(parts):
        if p + ahead < parts:
            spread_up(p + ahead)
        add(p)
    for p in range(up.shape[0]):
        give(p).wait()


def shards(nt, ns, u_old, u_init):
    depth, rows, cols = u_init.shape
    depth_c, rows_c, cols_c = depth // 2, rows // 2, cols // 2
    half = rows_c // 2
    whole_c = depth_c * ns
    width = 2 * cols_c
    solvers = width // 8
    groups = GROUPS
    span = nt // groups
    length = -(-half * depth_c // 128) * 128
    extended = depth + 2 * HALO
    rounds = max(1, (nt - 1).bit_length())
    steps = depth // BLOCK - 2

    wide = np.repeat(hartley(cols_c), 2, axis=0)
    zero = np.zeros_like(wide)
    forth = 0.125 * np.block([[wide, zero], [zero, wide]])
    back = np.block([[wide, wide], [wide, -wide]])
    ytab = np.stack([two_parts(forth), two_parts(back)])
    wave_x = hartley(rows_c)
    xtab = np.zeros((half * half, width), np.float32)
    for j in range(half):
        for x in range(half):
            xtab[j * half + x, :cols_c] = wave_x[2 * j, x]
            xtab[j * half + x, cols_c:] = wave_x[2 * j + 1, x]
    wave_z = hartley(whole_c).reshape(ns, depth_c, whole_c)
    late_c = BLOCK
    blocks = length // (half * late_c)
    sets = -(-ns // blocks)
    middles = 1 if depth_c > 2 * late_c else 0
    early_c = depth_c - (1 + middles) * late_c
    per_tile = length // (half * early_c) if early_c else 1
    tiles = -(-3 // per_tile) if early_c else 1
    early_sets = -(-ns // per_tile) if early_c else 0
    zearly = np.zeros((early_sets, length, half * whole_c))
    zlate = np.zeros((middles + 1, sets * blocks, half, late_c, half, whole_c))
    for j in range(half):
        for q in range(ns if early_c else 0):
            row = q % per_tile * half * early_c + j * early_c
            zearly[q // per_tile, row:row + early_c, j * whole_c:(j + 1) * whole_c] = wave_z[q, :early_c]
        for k in range(middles + 1):
            begin = early_c + k * late_c
            zlate[k, :ns, j, :, j] = wave_z[:, begin:begin + late_c]
    zearly = two_parts(zearly.reshape(early_sets * length, half * whole_c))
    zlate = np.stack([two_parts(part.reshape(sets * length, half * whole_c)) for part in zlate])
    wave = two_parts(hartley(whole_c))
    zback = np.block([[wave[0], wave[1]], [wave[0], np.zeros_like(wave[0])]])
    angle_z = 2.0 * np.cos(2.0 * np.pi * np.arange(whole_c) / whole_c)
    angle_x = 2.0 * np.cos(2.0 * np.pi * np.arange(rows_c) / rows_c)
    angle_y = 2.0 * np.cos(2.0 * np.pi * np.arange(cols_c) / cols_c)
    eigen = 0.25 * (
        angle_x.reshape(half, 2).T[:, None, :, None] + angle_y[None, :, None, None] + angle_z - 6.0
    )
    inv = (1.0 / (1.0 - 0.5 * step_length * diffusion * eigen)).astype(np.float32)
    inv = inv.reshape(width, half * whole_c)

    total = half * whole_c
    misc = np.zeros((4 * width, total), jnp.bfloat16)
    misc[:, :width] = ytab[0].reshape(4 * width, width)
    misc[:, width:2 * width] = ytab[1].reshape(4 * width, width)
    misc[:2 * whole_c, 2 * width:2 * width + 2 * whole_c] = zback
    half_tab = np.concatenate([misc, zearly.reshape(-1, total), zlate.reshape(-1, total)], axis=0)
    full_tab = np.zeros((width + half * half, total), np.float32)
    full_tab[:width], full_tab[width:, :width] = inv, xtab
    f32 = jnp.float32
    bf16 = jnp.bfloat16
    arrays = (u_old, u_init, half_tab, full_tab)
    handed = pl.pallas_call(
        functools.partial(kernel, nt, ns, groups),
        out_shape=(
            jax.ShapeDtypeStruct((5, extended, rows, cols), f32),
            jax.ShapeDtypeStruct((solvers, 3, 8, length), f32),
            jax.ShapeDtypeStruct(half_tab.shape, bf16),
            jax.ShapeDtypeStruct(full_tab.shape, f32),
        ),
        in_specs=[pl.BlockSpec(memory_space=pltpu.HBM)] * len(arrays),
        out_specs=(pl.BlockSpec(memory_space=pltpu.VMEM),) * 4,
        scratch_shapes=[
            pltpu.VMEM((5, extended, rows, cols), f32),
            pltpu.VMEM((4, extended, rows, cols), f32),
            pltpu.VMEM((4, extended, rows, cols), f32),
            pltpu.VMEM((3 * depth_c * rows, cols), f32),
            pltpu.VMEM((tiles, width, length), f32),
            pltpu.VMEM((span * ns, tiles, 8, length), f32),
            pltpu.VMEM((middles + 1, length, width), f32),
            pltpu.VMEM((middles + 1, width, length), f32),
            pltpu.VMEM((middles + 1, span * ns, 8, length), f32),
            pltpu.VMEM((span * ns, 3, 8, length), f32),
            pltpu.VMEM((8, half * whole_c), f32),
            pltpu.VMEM((8, half * whole_c), f32),
            pltpu.VMEM((RELAYS, BLOCK, rows, cols), f32),
            pltpu.SemaphoreType.DMA,
            pltpu.SemaphoreType.DMA((2,)),
            pltpu.SemaphoreType.DMA,
            pltpu.SemaphoreType.DMA,
            pltpu.SemaphoreType.DMA((2,)),
            pltpu.SemaphoreType.DMA((steps - max(0, early_c // BLOCK - 1) + 1,)),
            pltpu.SemaphoreType.DMA((2,)),
            pltpu.SemaphoreType.DMA((8,)),
            pltpu.SemaphoreType.REGULAR((rounds,)),
        ],
        compiler_params=pltpu.CompilerParams(
            collective_id=0, has_side_effects=True, vmem_limit_bytes=36000000
        ),
    )(*(pltpu.with_memory_space_constraint(a, pltpu.HBM) for a in arrays))
    return pl.pallas_call(
        finish,
        out_shape=jax.ShapeDtypeStruct((1, 5, depth, rows, cols), f32),
        in_specs=[pl.BlockSpec(memory_space=pltpu.VMEM)] * 4,
        out_specs=pl.BlockSpec(memory_space=pltpu.HBM),
        scratch_shapes=[
            pltpu.VMEM((3, length, width), f32),
            pltpu.VMEM((depth_c // 8, 3 * 8 * rows, cols), f32),
            pltpu.VMEM((depth_c // 8, 5, 16, rows, cols), f32),
            pltpu.SemaphoreType.DMA((depth_c // 8,)),
        ],
        compiler_params=pltpu.CompilerParams(vmem_limit_bytes=16000000),
    )(*handed)


def solution(mesh):
    return jax.shard_map(
        functools.partial(shards, mesh.shape["tm"], mesh.shape["space"]),
        mesh=mesh,
        in_specs=(P("tm", None, "space", None, None), P("space", None, None)),
        out_specs=P("tm", None, "space", None, None),
        check_vma=False,
    )
```

```python
import functools
import math

import jax
import jax.numpy as jnp
import numpy as np
from jax import lax
from jax.experimental import pallas as pl
from jax.experimental.pallas import tpu as pltpu
from jax.sharding import PartitionSpec as P

step_length = 0.4
diffusion = 1.0
reaction = 1.0
HALO = 5
BLOCK = 8
AHEAD = 2
RELAYS = 3
GROUPS = 2
MESH = pl.DeviceIdType.MESH


def basis_coefficients(nodes, chosen):
    polynomial = [1.0]
    for other, point in enumerate(nodes):
        if other == chosen:
            continue
        divisor = nodes[chosen] - point
        widened = [0.0] * (len(polynomial) + 1)
        for power, value in enumerate(polynomial):
            widened[power + 1] += value / divisor
            widened[power] -= value * point / divisor
        polynomial = widened
    return polynomial


def basis_value(nodes, chosen, where):
    result = 1.0
    for other, point in enumerate(nodes):
        if other != chosen:
            result *= (where - point) / (nodes[chosen] - point)
    return result


def node_tables():
    root = math.sqrt(3.0 / 7.0)
    fine_tau = [0.0, (1.0 - root) / 2.0, 0.5, (1.0 + root) / 2.0, 1.0]
    coarse_tau = [0.0, 0.5, 1.0]
    integ = []
    for j in range(4):
        row_values = []
        for k in range(5):
            polynomial = basis_coefficients(fine_tau, k)
            total = 0.0
            for power, value in enumerate(polynomial):
                total += (
                    value
                    * (fine_tau[j + 1] ** (power + 1) - fine_tau[j] ** (power + 1))
                    / (power + 1)
                )
            row_values.append(total)
        integ.append(row_values)
    interp = [[basis_value(coarse_tau, c, fine_tau[m]) for c in range(3)] for m in range(5)]
    spacing = [float(fine_tau[j + 1] - fine_tau[j]) for j in range(4)]
    return integ, spacing, interp


def hartley(length):
    counter = np.arange(length)
    phase = 2.0 * np.pi * (counter[:, None] * counter[None, :] % length) / length
    return (np.cos(phase) + np.sin(phase)) / math.sqrt(length)


def two_parts(table):
    upper = table.astype(jnp.bfloat16)
    lower = (table - upper.astype(np.float64)).astype(jnp.bfloat16)
    return np.stack([upper, lower])


def halves(value):
    upper = value.astype(jnp.bfloat16)
    return upper, (value - upper.astype(jnp.float32)).astype(jnp.bfloat16)


def product(a, b, dims):
    def one(x, y):
        return lax.dot_general(x, y, (dims, ((), ())), preferred_element_type=jnp.float32)

    return one(a[0], b[0]) + (one(a[0], b[1]) + one(a[1], b[0]))


def tables_of(half_tab, width, whole_c, middles, late):
    rows = 2 * width
    early = half_tab.shape[0] - 2 * rows - (middles + 1) * 2 * late

    def forth(i):
        return half_tab[pl.ds(i * rows, rows), pl.ds(0, width)]

    def back(i):
        return half_tab[pl.ds(i * rows, rows), pl.ds(width, width)]

    def z_back():
        return half_tab[pl.ds(0, 2 * whole_c), pl.ds(2 * width, 2 * whole_c)]

    def z_early(i):
        return half_tab[pl.ds(2 * rows + i * (early // 2), early // 2), :]

    def z_late(k, i):
        return half_tab[pl.ds(2 * rows + early + (2 * k + i) * late, late), :]

    return forth, back, z_back, z_early, z_late


def far_first(flip):
    hops = bin(flip[0]).count("1") + bin(flip[1] // 2).count("1")
    return -(flip[1] // 2), -hops, flip


def force(padded):
    field = padded[1:-1]
    rows, cols = field.shape[1:]
    near = padded[2:] + padded[:-2]
    near = near + (pltpu.roll(field, 1, 1) + pltpu.roll(field, rows - 1, 1))
    near = near + (pltpu.roll(field, 1, 2) + pltpu.roll(field, cols - 1, 2))
    linear = reaction - 6.0 * diffusion
    return diffusion * near + field * (linear - reaction * (field * field))


def kernel(
    nt, ns, groups,
    u_hbm, init_hbm, half_tab_hbm, full_tab_hbm,
    w, recv_2, half_tab, full_tab,
    u, corr, forces, restricted,
    send_a, recv_a, staged, send_l, recv_l, send_2, carry_out, carry_in,
    held,
    load_sem, table_sem, start_sem, early_send, edge_recv, start_recv, relay_sems,
    sems, known_sem,
):
    integ, spacing, _ = node_tables()
    h = step_length
    depth, rows, cols = init_hbm.shape
    depth_c, rows_c = depth // 2, rows // 2
    half = rows_c // 2
    width = staged.shape[1]
    length = send_2.shape[3]
    late_c = BLOCK
    blocks = length // (half * late_c)
    middles = 1 if depth_c > 2 * late_c else 0
    early_c = depth_c - (1 + middles) * late_c
    tiles = send_a.shape[0]
    whole_c = depth_c * ns
    extended = depth + 2 * HALO
    ytab, _, zback, zearly, zlate = tables_of(half_tab, width, whole_c, middles, -(-ns // blocks) * length)
    inv, xtab = full_tab.at[pl.ds(0, width)], full_tab.at[pl.ds(width, half * half), pl.ds(0, width)]
    solvers = width // 8
    span = nt // groups
    own = pl.ds(HALO, depth)
    t, s = lax.axis_index("tm"), lax.axis_index("space")
    group = t // span
    base = group * span
    above, below = lax.rem(s + 1, ns), lax.rem(s + ns - 1, ns)
    per = max(1, solvers // ns)
    lead = base + (span - per) // 2
    mine = (t - lead) * ns + s
    is_solver = (t >= lead) & (mine < solvers)
    all_solve = solvers == span * ns

    def place_of(a):
        return lead + a // ns, lax.rem(a, ns)

    barrier = pltpu.get_barrier_semaphore()

    def signal_along(sem, step):
        @pl.when(t + step < nt)
        def _():
            pl.semaphore_signal(sem, inc=1, device_id=(t + step, s), device_id_type=MESH)

        @pl.when(t >= step)
        def _():
            pl.semaphore_signal(sem, inc=1, device_id=(t - step, s), device_id_type=MESH)

    def sides(step):
        return jnp.where(t + step < nt, 1, 0) + jnp.where(t >= step, 1, 0)

    signal_along(barrier, 1)
    for i in range(1, ns):
        pl.semaphore_signal(
            barrier, inc=1, device_id=(t, lax.rem(s + i, ns)), device_id_type=MESH
        )
    load = pltpu.make_async_copy(u_hbm.at[0], u.at[:, own], load_sem)
    load.start()
    tables = [
        pltpu.make_async_copy(half_tab_hbm, half_tab, table_sem.at[0]),
        pltpu.make_async_copy(full_tab_hbm, full_tab, table_sem.at[1]),
    ]
    for copy in tables:
        copy.start()
    local_start = pltpu.make_async_copy(init_hbm, w.at[0, own], start_sem)

    @pl.when(t == 0)
    def _():
        local_start.start()

    with jax.named_scope("barrier"):
        pl.semaphore_wait(barrier, ns - 1 + sides(1))

    lows, highs = pl.ds(0, HALO), pl.ds(HALO + depth, HALO)
    first, last = pl.ds(0, HALO), pl.ds(depth - HALO, HALO)

    def remote(source, target, send, recv, place):
        return pltpu.make_async_remote_copy(
            src_ref=source, dst_ref=target, send_sem=send, recv_sem=recv,
            device_id=place, device_id_type=MESH,
        )

    after = jnp.minimum(t + 1, nt - 1)
    node = u_hbm.at[0, 4]
    steps = depth // BLOCK - 2
    doubles = early_c // BLOCK
    chunks = [(HALO + i * 2 * BLOCK, 2 * BLOCK) for i in range(doubles - 1)]
    singles = steps - 2 * len(chunks)
    chunks += [(HALO + (steps - singles + i) * BLOCK, BLOCK) for i in range(singles)]
    chunks.append((HALO + steps * BLOCK, depth - 2 * HALO - steps * BLOCK))
    relays = min(held.shape[0], max(0, singles - 1)) if nt > 4 else 0
    relayed = len(chunks) - 1 - relays

    def relays_of(to):
        return jnp.where(to == 1, relays, 0)

    def start_piece(sem, begin, size):
        return remote(
            node.at[pl.ds(begin, size)], w.at[0, pl.ds(HALO + begin, size)],
            early_send, sem, (after, s),
        )

    def chunk(i):
        return start_piece(start_recv.at[i], *chunks[i])

    def planes_wait(count, sem):
        whole = next(k for k in range(1, 6) if count % k == 0 and count // k <= extended)
        part = u.at[pl.ds(0, whole), pl.ds(0, count // whole)]
        pltpu.make_async_copy(part, part, sem).wait()

    start_edges = [start_piece(edge_recv.at[0], 0, HALO), start_piece(edge_recv.at[0], depth - HALO, HALO)]

    def edges(source, shift):
        return [
            remote(
                source.at[pl.ds(shift + depth - HALO, HALO)], w.at[0, lows],
                early_send, edge_recv.at[1], (t, above),
            ),
            remote(
                source.at[pl.ds(shift, HALO)], w.at[0, highs],
                early_send, edge_recv.at[1], (t, below),
            ),
        ]

    inits, passed = edges(init_hbm, 0), edges(w.at[0], HALO)
    halos = [
        remote(u_hbm.at[0, :, last], u.at[:, lows], early_send, load_sem, (t, above)),
        remote(u_hbm.at[0, :, first], u.at[:, highs], early_send, load_sem, (t, below)),
    ]

    mine_relayed, theirs_relayed = relays_of(t), relays_of(t + 1)

    @pl.when(t < nt - 1)
    def _():
        for copy in start_edges:
            copy.start()
        for i in range(len(chunks)):
            k = i - relayed
            if 0 <= k < relays:
                @pl.when(mine_relayed >= relays - k)
                def _(i=i, k=k):
                    begin, size = chunks[i]
                    remote(
                        node.at[pl.ds(begin, size)], held.at[k], early_send, relay_sems.at[0], (t - 1, s)
                    ).start()

                @pl.when(mine_relayed < relays - k)
                def _(i=i):
                    chunk(i).start()
            else:
                chunk(i).start()

    for copy in halos:
        copy.start()

    @pl.when(t == 0)
    def _():
        for copy in inits:
            copy.start()

    signal_along(known_sem.at[0], 1)
    rounds = known_sem.shape[0]

    def hear(i):
        pl.semaphore_wait(known_sem.at[i], sides(2 ** i))
        if i + 1 < rounds:
            signal_along(known_sem.at[i + 1], 2 ** (i + 1))

    with jax.named_scope("w_edges"):
        @pl.when(t > 0)
        def _():
            planes_wait(2 * HALO, edge_recv.at[0])
            for copy in passed:
                copy.start()

    if rounds > 1:
        hear(0)

    with jax.named_scope("w_halo"):
        pltpu.make_async_copy(u, u, load_sem).wait()

    if rounds > 2:
        hear(1)
    for count in range(1, relays + 1):
        @pl.when(theirs_relayed == count)
        def _(count=count):
            planes_wait(count * BLOCK, relay_sems.at[0])
            for k in range(relays - count, relays):
                begin, size = chunks[relayed + k]
                remote(
                    held.at[k], w.at[0, pl.ds(HALO + begin, size)], relay_sems.at[1],
                    start_recv.at[relayed + k], (t + 2, s),
                ).start()

    def fold_block(i, carry):
        z = 1 + i * BLOCK
        parts = [force(u[k, pl.ds(z - 1, BLOCK + 2)]) for k in range(5)]
        for j in range(4):
            total = None
            for k in range(5):
                weight = h * integ[j][k] - (h * spacing[j] if j == k else 0.0)
                term = weight * parts[k]
                total = term if total is None else total + term
            corr[j, pl.ds(z, BLOCK)] = total
        return carry

    with jax.named_scope("fold"):
        lax.fori_loop(0, (depth + 2 * HALO - 2) // BLOCK, fold_block, 0)

    for i in range(2, rounds - 1):
        hear(i)

    @pl.when(t == 0)
    def _():
        local_start.wait()

    planes_wait(2 * HALO, edge_recv.at[1])

    def advance(m, padded, here):
        now = force(padded)
        forces[m, here] = now
        result = padded[1:-1] + (h * spacing[m]) * now + corr[m, here]
        w[m + 1, here] = result
        return result

    plane = rows * depth_c

    def step(begin, count):
        reached = None
        for m in range(5):
            at = begin - m
            if m == 0:
                padded = w[0, pl.ds(at - 1, count + 2)]
            else:
                padded = jnp.concatenate([w[m, pl.ds(at - 1, 2)], reached], axis=0)
            if m < 4:
                reached = advance(m, padded, pl.ds(at, count))
        here = pl.ds(at, count)
        now, end = force(padded), padded[1:-1]
        middle = w[2, here]
        olds = [forces[m, here] for m in range(4)] + [now]
        outs = []
        for a in range(2):
            total = (w[0, here] - middle) if a == 0 else (middle - end)
            for m in range(5):
                total = total + (h * (integ[2 * a][m] + integ[2 * a + 1][m])) * olds[m]
            outs.append(total)
        outs.append(end - u[4, here])
        for f in range(3):
            pair = outs[f].reshape(count // 2, 2, rows, cols)
            pair = pair[:, 0] + pair[:, 1]
            to = f * plane + (at - HALO) // 2 * rows
            if not isinstance(to, int):
                to = pl.multiple_of(to, 8)
            restricted[pl.ds(to, count // 2 * rows), :] = pair.reshape(count // 2 * rows, cols)

    with jax.named_scope("prologue"):
        for m in range(4):
            count = BLOCK - 2 * m
            advance(m, w[m, pl.ds(m, count + 2)], pl.ds(1 + m, count))

    def main_step(begin, size):
        @pl.when(t > 0)
        def _():
            for i, (first_z, count) in enumerate(chunks):
                if begin <= first_z and first_z + count <= begin + size:
                    chunk(i).wait_recv()

        step(begin + 4, size)

    def transformed(begin, count):
        slabs = []
        for x in range(rows_c):
            fields = []
            for f in range(3):
                at = f * plane + begin * rows + 2 * x
                even = restricted[pl.ds(at, count, stride=rows), :]
                odd = restricted[pl.ds(at + 1, count, stride=rows), :]
                fields.append(even + odd)
            slabs.append(jnp.concatenate(fields, axis=0))
        pairs = [
            jnp.concatenate([slabs[x] + slabs[x + half], slabs[x] - slabs[x + half]], axis=1)
            for x in range(half)
        ]
        turned = product(halves(jnp.concatenate(pairs, axis=0)), (ytab(0), ytab(1)), ((1,), (0,)))
        parts = [turned[x * 3 * count:(x + 1) * 3 * count] for x in range(half)]
        mixed = []
        for j in range(half):
            total = None
            for x in range(half):
                term = xtab[pl.ds(j * half + x, 1), :] * parts[x]
                total = term if total is None else total + term
            mixed.append(total)
        return [
            jnp.concatenate([mixed[j][f * count:(f + 1) * count] for j in range(half)], axis=0)
            for f in range(3)
        ]

    slot = s * span + (t - base)

    tau = t - base
    paired = all_solve and span & (span - 1) == 0 and ns & (ns - 1) == 0

    def flipped(value, mask):
        for bit in range(mask.bit_length()):
            if mask >> bit & 1:
                value = value + (1 - 2 * (value // 2 ** bit % 2)) * 2 ** bit
        return value

    def flips():
        return sorted(((a, b) for a in range(span) for b in range(ns) if a or b), key=far_first)

    def spread(source_of, target, sem):
        def go(a, to_t, to_s):
            remote(
                source_of(pl.ds(pl.multiple_of(a * 8, 8), 8)), target.at[slot],
                sems.at[0], sems.at[sem], (to_t, to_s),
            ).start()

        if paired:
            for flip_t, flip_s in flips():
                to_tau, to_s = flipped(tau, flip_t), flipped(s, flip_s)
                go(to_tau * ns + to_s, base + to_tau, to_s)
        else:
            def body(a, carry):
                to_t, to_s = place_of(a)

                @pl.when((to_t != t) | (to_s != s))
                def _():
                    go(a, to_t, to_s)

                return carry

            lax.fori_loop(0, solvers, body, 0)

    def late(k):
        high = half * late_c
        for f, field in enumerate(transformed(early_c + k * late_c, late_c)):
            staged[k, pl.ds(pl.multiple_of(lax.rem(f + s, blocks) * high, 8), high), :] = field
        for f in range(3, blocks):
            staged[k, pl.ds(pl.multiple_of(lax.rem(f + s, blocks) * high, 8), high), :] = jnp.zeros(
                (high, width), jnp.float32
            )
        send_l[k] = jnp.transpose(staged[k])

    with jax.named_scope("steps"):
        for i in range(doubles):
            main_step(HALO + i * 2 * BLOCK, 2 * BLOCK)

    with jax.named_scope("fwd_a"):
        for copy in tables:
            copy.wait()
        if early_c > 0:
            together = transformed(0, early_c)
            filled = half * early_c
            per_tile = length // filled
            for i in range(tiles):
                parts = together[i * per_tile:(i + 1) * per_tile]
                if len(parts) * filled < length:
                    parts.append(jnp.zeros((length - len(parts) * filled, width), jnp.float32))
                send_a[i] = jnp.transpose(jnp.concatenate(parts, axis=0))

    hear(rounds - 1)
    def issue_early():
        spread(lambda r: send_a.at[:, r], recv_a, 1)

    if early_c > 0:
        with jax.named_scope("issue_a"):
            pl.when(t > 0)(issue_early)

    with jax.named_scope("steps_m"):
        for i in range(2 * doubles, steps):
            main_step(HALO + i * BLOCK, BLOCK)

    if middles:
        with jax.named_scope("fwd_m"):
            late(0)
        if early_c > 0:
            pl.when(t == 0)(issue_early)
        with jax.named_scope("issue_m"):
            spread(lambda r: send_l.at[0, r], recv_l.at[0], 6)

    with jax.named_scope("w_final"):
        @pl.when(t > 0)
        def _():
            chunk(len(chunks) - 1).wait_recv()

    with jax.named_scope("tail"):
        step(HALO + 4 + steps * BLOCK, 2 * BLOCK)

    with jax.named_scope("fwd_b"):
        late(middles)
    with jax.named_scope("issue_b"):
        spread(lambda r: send_l.at[middles, r], recv_l.at[middles], 7)

    with jax.named_scope("sent"):
        @pl.when(t < nt - 1)
        def _():
            planes_wait(12 * HALO + depth, early_send)

        @pl.when(t == nt - 1)
        def _():
            planes_wait(12 * HALO, early_send)

        for count in range(1, relays + 1):
            @pl.when(theirs_relayed == count)
            def _(count=count):
                planes_wait(count * BLOCK, relay_sems.at[1])

    def when_solver(body):
        if all_solve:
            body()
        else:
            pl.when(is_solver)(body)

    def bytes_wait(ref, count, sem):
        if count > 0:
            part = ref.at[pl.ds(0, count)]
            pltpu.make_async_copy(part, part, sem).wait()

    def forward_sent(count):
        units = count * ((tiles if early_c > 0 else 0) + middles + 1)
        part = restricted.at[pl.ds(0, 8 * units)]
        pltpu.make_async_copy(part, part, sems.at[0]).wait()

    def carry_copy(to_t):
        return remote(carry_out, carry_in, sems.at[4], sems.at[5], (to_t, s))

    def solve():
        at = pl.multiple_of(mine * 8, 8)
        if early_c > 0:
            recv_a[slot] = send_a[:, pl.ds(at, 8)]
        for k in range(middles + 1):
            recv_l[k, slot] = send_l[k, pl.ds(at, 8), :]
        factor = inv[pl.ds(at, 8), :]
        spectra = None
        tall = span * 8
        if early_c > 0:
            with jax.named_scope("w_recv_a"):
                bytes_wait(recv_a, span * ns - 1, sems.at[1])
            with jax.named_scope("z_a"):
                filled = half * early_c
                per_tile = length // filled
                lane = lax.broadcasted_iota(jnp.int32, (tall, length), 1) // filled
                fields = []
                for f in range(3):
                    columns = []
                    for k in range(-(-ns // per_tile)):
                        chosen = jnp.zeros((tall, length), jnp.float32)
                        for g in range(min(per_tile, ns - k * per_tile)):
                            q = k * per_tile + g
                            value = recv_a[pl.ds(q * span, span), f // per_tile].reshape(tall, length)
                            shift = (g - f % per_tile) * filled % length
                            if shift:
                                value = pltpu.roll(value, shift, 1)
                            chosen = jnp.where(lane == g, value, chosen)
                        columns.append(chosen)
                    fields.append(jnp.concatenate(columns, axis=1))
                spectra = product(halves(jnp.concatenate(fields, axis=0)), (zearly(0), zearly(1)), ((1,), (0,)))

        def late_part(k):
            high = half * late_c
            arrived = [recv_l[k, pl.ds(q * span, span)].reshape(tall, length) for q in range(ns)]
            lane = lax.broadcasted_iota(jnp.int32, (tall, length), 1) // high
            fields = []
            for f in range(3):
                columns = []
                for c in range(-(-ns // blocks)):
                    chosen = jnp.zeros((tall, length), jnp.float32)
                    for q in range(c * blocks, min(ns, (c + 1) * blocks)):
                        chosen = jnp.where(lane == (f + q) % blocks, arrived[q], chosen)
                    if f > 0:
                        chosen = pltpu.roll(chosen, length - high * f, 1)
                    columns.append(chosen)
                fields.append(jnp.concatenate(columns, axis=1))
            return product(halves(jnp.concatenate(fields, axis=0)), (zlate(k, 0), zlate(k, 1)), ((1,), (0,)))

        if middles:
            with jax.named_scope("w_recv_m"):
                bytes_wait(recv_l.at[0], span * ns - 1, sems.at[6])
            with jax.named_scope("z_m"):
                more = late_part(0)
                spectra = more if spectra is None else spectra + more
        with jax.named_scope("w_recv_b"):
            bytes_wait(recv_l.at[middles], span * ns - 1, sems.at[7])
        with jax.named_scope("solve"):
            more = late_part(middles)
            spectra = more if spectra is None else spectra + more
            height = span * 8

            if groups > 1:
                carry_in_zero = group == 0

                @pl.when(carry_in_zero)
                def _():
                    carry_in[...] = jnp.zeros(carry_in.shape, jnp.float32)

                @pl.when(group > 0)
                def _():
                    carry_copy(t).wait_recv()

                begin = carry_in[...]
            else:
                begin = jnp.zeros(factor.shape, jnp.float32)
            fields = [[], [], []]
            for n in range(span):
                part = [spectra[f * height + n * 8:f * height + n * 8 + 8] for f in range(3)]
                middle = (begin + part[0]) * factor
                finish = (middle + part[1]) * factor
                for f, value in enumerate((begin, middle, finish)):
                    fields[f].append(value)
                begin = finish + part[2]
            if groups > 1:
                carry_out[...] = begin

                @pl.when(group < groups - 1)
                def _():
                    carry_copy(t + span).start()

            rows_all = jnp.concatenate(
                [
                    jnp.concatenate([value[:, j * whole_c:(j + 1) * whole_c] for field in fields for value in field], axis=0)
                    for j in range(half)
                ],
                axis=0,
            )
            upper, lower = halves(rows_all)
            wide = lax.dot_general(
                jnp.concatenate([upper, lower], axis=1), zback(), (((1,), (0,)), ((), ())),
                preferred_element_type=jnp.float32,
            )
            back = wide[:, :whole_c] + wide[:, whole_c:]
            turned = []
            for j in range(half):
                part = back[j * 3 * height:(j + 1) * 3 * height]
                turned.append(pltpu.roll(part, j * depth_c, 1) if j else part)
            lane = lax.broadcasted_iota(jnp.int32, (3 * height, length), 1) // depth_c
            for q in range(ns):
                message = turned[half - 1]
                for j in range(half - 1):
                    message = jnp.where(lane == (q + j) % ns, turned[j], message)
                for f in range(3):
                    send_2[pl.ds(q * span, span), f] = message[f * height:(f + 1) * height].reshape(span, 8, length)

        peers = span * ns

        def go(to_tau, to_s):
            remote(
                send_2.at[to_s * span + to_tau], recv_2.at[mine], sems.at[2], sems.at[3],
                (base + to_tau, to_s),
            ).start()

        with jax.named_scope("issue2"):
            if paired:
                for flip_t, flip_s in flips():
                    go(flipped(tau, flip_t), flipped(s, flip_s))
            else:
                def give(i, carry):
                    other = lax.rem(slot + i, peers)
                    go(lax.rem(other, span), other // span)
                    return carry

                lax.fori_loop(1, peers, give, 0)
        recv_2[mine] = send_2[slot]
        forward_sent(solvers - 1)
        with jax.named_scope("w_recv2"):
            bytes_wait(recv_2, solvers - 1, sems.at[3])

    when_solver(solve)
    if not all_solve:
        @pl.when(jnp.logical_not(is_solver))
        def _():
            forward_sent(solvers)
            with jax.named_scope("w_recv2"):
                bytes_wait(recv_2, solvers, sems.at[3])

    def sent():
        bytes_wait(send_2, span * ns - 1, sems.at[2])
        if groups > 1:
            @pl.when(group < groups - 1)
            def _():
                carry_copy(t).wait_send()

    when_solver(sent)


def finish(w, recv, half_tab, full_tab, out, returned, up, result, sems):
    _, _, interp = node_tables()
    depth, rows, cols = out.shape[2:]
    depth_c, rows_c = depth // 2, rows // 2
    half = rows_c // 2
    solvers, _, _, length = recv.shape
    count = depth_c // up.shape[0]
    s = lax.axis_index("space")
    slabs = length // depth_c
    width = solvers * 8
    _, ytab, _, _, _ = tables_of(half_tab, width, length, 0, 0)
    xtab = full_tab.at[pl.ds(width, half * half), pl.ds(0, width)]
    for f in range(3):
        returned[f] = jnp.transpose(recv[:, f].reshape(solvers * 8, length))
    places = [lax.rem(s + j, slabs) * depth_c for j in range(half)]

    def give(p):
        return pltpu.make_async_copy(result.at[p], out.at[0, :, pl.ds(p * 2 * count, 2 * count)], sems.at[p])

    def spread_up(p):
        mixed = [
            jnp.concatenate(
                [returned[f, pl.ds(pl.multiple_of(places[j] + p * count, 8), count), :] for f in range(3)], axis=0
            )
            for j in range(half)
        ]
        parts = []
        for x in range(half):
            total = None
            for j in range(half):
                term = xtab[pl.ds(j * half + x, 1), :] * mixed[j]
                total = term if total is None else total + term
            parts.append(total)
        coarse = product(halves(jnp.concatenate(parts, axis=0)), (ytab(0), ytab(1)), ((1,), (1,)))
        high = 3 * count
        for x in range(rows_c):
            part = coarse[(x % half) * high:(x % half + 1) * high, (x // half) * cols:(x // half + 1) * cols]
            for side in range(2):
                up[p, pl.ds(2 * x + side, high, stride=rows), :] = part

    def add(p):
        for z in range(count):
            fields = [up[p, pl.ds((f * count + z) * rows, rows), :] for f in range(3)]
            for m in range(5):
                total = None
                for c in range(3):
                    if abs(interp[m][c]) < 1e-14:
                        continue
                    term = fields[c]
                    if abs(interp[m][c] - 1.0) > 1e-14:
                        term = interp[m][c] * term
                    total = term if total is None else total + term
                for side in range(2):
                    result[p, m, 2 * z + side] = w[m, HALO + 2 * (p * count + z) + side] + total
        give(p).start()

    parts = up.shape[0]
    ahead = min(AHEAD, parts)
    for p in range(ahead):
        spread_up(p)
    for p in range(parts):
        if p + ahead < parts:
            spread_up(p + ahead)
        add(p)
    for p in range(up.shape[0]):
        give(p).wait()


def shards(nt, ns, u_old, u_init):
    depth, rows, cols = u_init.shape
    depth_c, rows_c, cols_c = depth // 2, rows // 2, cols // 2
    half = rows_c // 2
    whole_c = depth_c * ns
    width = 2 * cols_c
    solvers = width // 8
    groups = GROUPS
    span = nt // groups
    length = -(-half * depth_c // 128) * 128
    extended = depth + 2 * HALO
    rounds = max(1, (nt - 1).bit_length())
    steps = depth // BLOCK - 2

    wide = np.repeat(hartley(cols_c), 2, axis=0)
    zero = np.zeros_like(wide)
    forth = 0.125 * np.block([[wide, zero], [zero, wide]])
    back = np.block([[wide, wide], [wide, -wide]])
    ytab = np.stack([two_parts(forth), two_parts(back)])
    wave_x = hartley(rows_c)
    xtab = np.zeros((half * half, width), np.float32)
    for j in range(half):
        for x in range(half):
            xtab[j * half + x, :cols_c] = wave_x[2 * j, x]
            xtab[j * half + x, cols_c:] = wave_x[2 * j + 1, x]
    wave_z = hartley(whole_c).reshape(ns, depth_c, whole_c)
    late_c = BLOCK
    blocks = length // (half * late_c)
    sets = -(-ns // blocks)
    middles = 1 if depth_c > 2 * late_c else 0
    early_c = depth_c - (1 + middles) * late_c
    per_tile = length // (half * early_c) if early_c else 1
    tiles = -(-3 // per_tile) if early_c else 1
    early_sets = -(-ns // per_tile) if early_c else 0
    zearly = np.zeros((early_sets, length, half * whole_c))
    zlate = np.zeros((middles + 1, sets * blocks, half, late_c, half, whole_c))
    for j in range(half):
        for q in range(ns if early_c else 0):
            row = q % per_tile * half * early_c + j * early_c
            zearly[q // per_tile, row:row + early_c, j * whole_c:(j + 1) * whole_c] = wave_z[q, :early_c]
        for k in range(middles + 1):
            begin = early_c + k * late_c
            zlate[k, :ns, j, :, j] = wave_z[:, begin:begin + late_c]
    zearly = two_parts(zearly.reshape(early_sets * length, half * whole_c))
    zlate = np.stack([two_parts(part.reshape(sets * length, half * whole_c)) for part in zlate])
    wave = two_parts(hartley(whole_c))
    zback = np.block([[wave[0], wave[1]], [wave[0], np.zeros_like(wave[0])]])
    angle_z = 2.0 * np.cos(2.0 * np.pi * np.arange(whole_c) / whole_c)
    angle_x = 2.0 * np.cos(2.0 * np.pi * np.arange(rows_c) / rows_c)
    angle_y = 2.0 * np.cos(2.0 * np.pi * np.arange(cols_c) / cols_c)
    eigen = 0.25 * (
        angle_x.reshape(half, 2).T[:, None, :, None] + angle_y[None, :, None, None] + angle_z - 6.0
    )
    inv = (1.0 / (1.0 - 0.5 * step_length * diffusion * eigen)).astype(np.float32)
    inv = inv.reshape(width, half * whole_c)

    total = half * whole_c
    misc = np.zeros((4 * width, total), jnp.bfloat16)
    misc[:, :width] = ytab[0].reshape(4 * width, width)
    misc[:, width:2 * width] = ytab[1].reshape(4 * width, width)
    misc[:2 * whole_c, 2 * width:2 * width + 2 * whole_c] = zback
    half_tab = np.concatenate([misc, zearly.reshape(-1, total), zlate.reshape(-1, total)], axis=0)
    full_tab = np.zeros((width + half * half, total), np.float32)
    full_tab[:width], full_tab[width:, :width] = inv, xtab
    f32 = jnp.float32
    bf16 = jnp.bfloat16
    arrays = (u_old, u_init, half_tab, full_tab)
    handed = pl.pallas_call(
        functools.partial(kernel, nt, ns, groups),
        out_shape=(
            jax.ShapeDtypeStruct((5, extended, rows, cols), f32),
            jax.ShapeDtypeStruct((solvers, 3, 8, length), f32),
            jax.ShapeDtypeStruct(half_tab.shape, bf16),
            jax.ShapeDtypeStruct(full_tab.shape, f32),
        ),
        in_specs=[pl.BlockSpec(memory_space=pltpu.HBM)] * len(arrays),
        out_specs=(pl.BlockSpec(memory_space=pltpu.VMEM),) * 4,
        scratch_shapes=[
            pltpu.VMEM((5, extended, rows, cols), f32),
            pltpu.VMEM((4, extended, rows, cols), f32),
            pltpu.VMEM((4, extended, rows, cols), f32),
            pltpu.VMEM((3 * depth_c * rows, cols), f32),
            pltpu.VMEM((tiles, width, length), f32),
            pltpu.VMEM((span * ns, tiles, 8, length), f32),
            pltpu.VMEM((middles + 1, length, width), f32),
            pltpu.VMEM((middles + 1, width, length), f32),
            pltpu.VMEM((middles + 1, span * ns, 8, length), f32),
            pltpu.VMEM((span * ns, 3, 8, length), f32),
            pltpu.VMEM((8, half * whole_c), f32),
            pltpu.VMEM((8, half * whole_c), f32),
            pltpu.VMEM((RELAYS, BLOCK, rows, cols), f32),
            pltpu.SemaphoreType.DMA,
            pltpu.SemaphoreType.DMA((2,)),
            pltpu.SemaphoreType.DMA,
            pltpu.SemaphoreType.DMA,
            pltpu.SemaphoreType.DMA((2,)),
            pltpu.SemaphoreType.DMA((steps - max(0, early_c // BLOCK - 1) + 1,)),
            pltpu.SemaphoreType.DMA((2,)),
            pltpu.SemaphoreType.DMA((8,)),
            pltpu.SemaphoreType.REGULAR((rounds,)),
        ],
        compiler_params=pltpu.CompilerParams(
            collective_id=0, has_side_effects=True, vmem_limit_bytes=36000000
        ),
    )(*(pltpu.with_memory_space_constraint(a, pltpu.HBM) for a in arrays))
    return pl.pallas_call(
        finish,
        out_shape=jax.ShapeDtypeStruct((1, 5, depth, rows, cols), f32),
        in_specs=[pl.BlockSpec(memory_space=pltpu.VMEM)] * 4,
        out_specs=pl.BlockSpec(memory_space=pltpu.HBM),
        scratch_shapes=[
            pltpu.VMEM((3, length, width), f32),
            pltpu.VMEM((depth_c // 8, 3 * 8 * rows, cols), f32),
            pltpu.VMEM((depth_c // 8, 5, 16, rows, cols), f32),
            pltpu.SemaphoreType.DMA((depth_c // 8,)),
        ],
        compiler_params=pltpu.CompilerParams(vmem_limit_bytes=16000000),
    )(*handed)


def solution(mesh):
    return jax.shard_map(
        functools.partial(shards, mesh.shape["tm"], mesh.shape["space"]),
        mesh=mesh,
        in_specs=(P("tm", None, "space", None, None), P("space", None, None)),
        out_specs=P("tm", None, "space", None, None),
        check_vma=False,
    )
```
